256 devices in a mesh: ep: 64 (over z, x, core), tp: 4 (over y).
Axes of the slice: x: 4, y: 4, z: 8, core: 2. Of those that a mesh axis runs over, the one named last changes fastest.
Arguments:
- hidden: bfloat16 [4096, 2880], P('ep'), may hold values from -0.59765625 to 0.59765625
- queries: bfloat16 [4096, 2048], P('ep', 'tp'), may hold values from -160 to 160
- new_keys: bfloat16 [4096, 256], P('ep', 'tp'), may hold values from -6 to 6
- new_values: bfloat16 [4096, 256], P('ep', 'tp'), may hold values from -6 to 6
- key_cache: bfloat16 [512, 4, 64, 1024], P('ep', 'tp'), may hold values from -6 to 6
- value_cache: bfloat16 [512, 4, 64, 1024], P('ep', 'tp'), may hold values from -6 to 6
- cache_lengths: int32 [512], P('ep'), may hold values from 16 to 1024
- w_out: bfloat16 [2048, 2880], P('tp'), may hold values from -0.125 to 0.125
- w_router: bfloat16 [2880, 64], replicated, may hold values from -0.109375 to 0.109375
- routes: int32 [4096, 4], P('ep'), may hold values from 0 to 63, all different within a row; in each aligned block of 16 rows (0 to 15, 16 to 31, ...) at most 2 rows name the same one
- w_gate: bfloat16 [64, 2880, 1536], P('ep', None, 'tp'), may hold values from -0.109375 to 0.109375
- w_up: bfloat16 [64, 2880, 1536], P('ep', None, 'tp'), may hold values from -0.109375 to 0.109375
- w_down: bfloat16 [64, 1536, 2880], P('ep', 'tp'), may hold values from -0.15625 to 0.15625
Outputs:
- layer_out: bfloat16 [4096, 2880], P(('ep', 'tp'))
The draws below stay inside these ranges and needn't reach their ends.
Inputs may be any that keep to these rules, and one draw needn't show every extreme that they name: `routes`: each token names 4 different experts; in each aligned block of 16 tokens no expert is named by more than 2 tokens, and in some blocks one expert is named by exactly 2.
All inputs are finite; a program needn't handle non-finite values.
Results may differ from the reference program's by a relative error of at most 0.02.
Values may be sent and summed in bfloat16 or wider, within the bound.
A program may use at most 64 MiB of HBM per device.

```python
import math
import jax
import jax.numpy as jnp
import numpy as np
from jax import lax

D = 2880
HEADS = 32
KV_HEADS = 4
HEAD_DIM = 64
FF = 1536
TOP = 4
SEQ_DEV = 8
LEN = 1024
EXPERTS = 64
SEQS = 512
TOKENS = 4096
TOK_EP = 64
BLOCK = 16
CAP = 2
N_EP = 64
N_TP = 4


def draw_queries(key, part):
    shape_q = (TOKENS, HEADS * HEAD_DIM)
    values = jnp.clip(jax.random.normal(jax.random.fold_in(key, 1), shape_q, jnp.float32), -6.0, 6.0)
    return values.astype(jnp.bfloat16)


def draw_key_cache(key, part):
    base_draw = jax.random.normal(jax.random.fold_in(key, 3), (SEQS, KV_HEADS, HEAD_DIM, LEN), jnp.float32)
    base_draw = jnp.clip(base_draw, -6.0, 6.0)
    return base_draw.astype(jnp.bfloat16)


def place_ends(array, stream_key, low, high):
    dims = array.shape
    index_at = [jax.random.randint(jax.random.fold_in(stream_key, axis), (), 0, dims[axis]) for axis in range(len(dims))]
    array = array.at[tuple(index_at)].set(low)
    longest = dims.index(max(dims))
    index_at[longest] = (index_at[longest] + 1) % dims[longest]
    return array.at[tuple(index_at)].set(high)


def levels(key, dims, cuts, low, largest):
    gain = 1.0
    for axis_at, parts in cuts:
        steps = jax.random.uniform(jax.random.fold_in(jax.random.fold_in(key, 6), axis_at), (parts,), jnp.float32, low / len(cuts), largest / len(cuts))
        gain = gain * jnp.repeat(jnp.exp(steps), dims[axis_at] // parts).reshape((-1,) + (1,) * (len(dims) - 1 - axis_at))
    return gain


def deal_out(stream_key, own, number, rows, amount, top, reach, lean):
    ranking = jax.random.permutation(stream_key, amount)
    packed, common = portions_of(amount, rows * top, reach, lean, True), portions_of(amount, rows * top, reach, lean, False)
    places = jnp.arange(amount)

    def named(lengths, turn):
        used = int((lengths > 0).sum())
        fixed = max(1, used // 4)
        passed = fixed + (places - fixed + turn * (used - fixed)) % max(1, amount - fixed)
        return jnp.zeros((amount,), jnp.int32).at[ranking[jnp.where(places < fixed, places, passed)]].set(jnp.asarray(lengths, jnp.int32))

    lengths = jnp.where(number % 4 == 0, named(packed, number // 4), named(common, number - number // 4 - 1))
    mixed = jax.random.permutation(jax.random.fold_in(own, 3), amount)
    giver, receiver = mixed[0:amount // 2 * 2:2], mixed[1:amount // 2 * 2:2]
    slack = jnp.minimum(lengths[giver] - 1, reach - lengths[receiver]) // 2
    slack = jnp.where((giver == ranking[0]) | (receiver == ranking[0]) | (lengths[receiver] == 0), 0, jnp.maximum(slack, 0))
    passed = jax.random.randint(jax.random.fold_in(own, 4), (amount // 2,), 0, 1 << 20) % (slack + 1)
    lengths = lengths.at[giver].add(-passed).at[receiver].add(passed)
    items = jnp.searchsorted(jnp.cumsum(lengths), jnp.arange(rows * top), side="right").astype(jnp.int32)
    table = items.reshape(top, rows).T
    table = table[jax.random.permutation(jax.random.fold_in(own, 1), rows)]
    turn = jax.random.randint(jax.random.fold_in(own, 2), (rows, 1), 0, top)
    return jnp.take_along_axis(table, (jnp.arange(top)[None, :] + turn) % top, axis=1)


def portions_of(count, total, most, slope, full):
    weights = [(1 << 20) // math.isqrt(standing ** slope) + 1 for standing in range(1, count + 1)]
    largest = most if full else min(most, max(-(-total // count), total * weights[0] // sum(weights)))
    least = 1 if total - largest >= count - 1 else 0
    holding, rest = [largest] + [least] * (count - 1), total - largest - least * (count - 1)
    while rest > 0:
        movable = [i for i in range(1, count) if holding[i] < largest] or [i for i in range(1, count) if holding[i] < most]
        mass, left = sum([weights[i] for i in movable]), rest
        for i in movable:
            extra = min(most - holding[i], max(1, left * weights[i] // mass), rest)
            holding[i] = holding[i] + extra
            rest = rest - extra
    return np.array(holding)


def centred(key, dims, width, limit, split=(), kind=jnp.bfloat16):
    values = jax.random.normal(key, dims, jnp.float32) * width
    if len(split) > 0:
        values = levels(key, dims, split, -0.22, 0.18) * values
    return jnp.clip(values, min=-limit, max=limit).astype(kind)


def setup_inputs(seed: int = 0) -> dict:
    keys = jax.random.split(jax.random.key(seed), 14)
    hidden = centred(keys[0], (TOKENS, D), 0.1, 0.59765625, ((0, 64),))
    queries = draw_queries(jax.random.fold_in(keys[13], 71), 0)
    new_keys = centred(keys[2], (TOKENS, KV_HEADS * HEAD_DIM), 1.0, 6.0, ((0, 64), (1, 4)))
    new_values = centred(keys[3], (TOKENS, KV_HEADS * HEAD_DIM), 1.0, 6.0, ((0, 64), (1, 4)))
    key_cache = draw_key_cache(jax.random.fold_in(keys[13], 71), 0)
    value_cache = centred(keys[5], (SEQS, KV_HEADS, HEAD_DIM, LEN), 1.0, 6.0, ((0, 64), (1, 4)))
    cache_lengths = place_ends(jax.random.randint(keys[6], (SEQS,), 16, LEN + 1), jax.random.fold_in(keys[6], 1), 16, LEN).astype(jnp.int32)
    w_out = centred(keys[7], (HEADS * HEAD_DIM, D), (HEADS * HEAD_DIM) ** -0.5, 0.125, ((0, 4),))
    w_router = centred(keys[8], (D, EXPERTS), D ** -0.5, 0.109375)
    routes_keys = jax.random.split(jax.random.fold_in(keys[9], 1), TOKENS // BLOCK)
    routes_turns = jax.random.permutation(jax.random.fold_in(keys[9], 3), TOKENS // BLOCK)
    routes = jax.vmap(lambda own, number: deal_out(jax.random.fold_in(keys[9], 2), own, number, BLOCK, EXPERTS, TOP, CAP, 2))(routes_keys, routes_turns).reshape((TOKENS, TOP))
    w_gate = centred(keys[10], (EXPERTS, D, FF), D ** -0.5, 0.109375, ((0, 64), (2, 4)))
    w_up = centred(keys[11], (EXPERTS, D, FF), D ** -0.5, 0.109375, ((0, 64), (2, 4)))
    w_down = centred(keys[12], (EXPERTS, FF, D), FF ** -0.5, 0.15625, ((0, 64), (1, 4)))
    return dict(hidden=hidden, queries=queries, new_keys=new_keys, new_values=new_values, key_cache=key_cache, value_cache=value_cache, cache_lengths=cache_lengths, w_out=w_out, w_router=w_router, routes=routes, w_gate=w_gate, w_up=w_up, w_down=w_down)


def attend_block(queries, new_keys, new_values, key_cache, value_cache, cache_lengths):
    seq_count, kv_count, head_dim, length = key_cache.shape
    new_count = queries.shape[0] // seq_count
    group_size = queries.shape[1] // (kv_count * head_dim)
    row_count = new_count * group_size
    scale = head_dim ** (-0.5)
    query_block = queries.astype(jnp.float32).reshape(seq_count, new_count, kv_count, group_size, head_dim)
    query_block = query_block.transpose(0, 2, 1, 3, 4).reshape(seq_count, kv_count, row_count, head_dim)
    fresh_keys = new_keys.astype(jnp.float32).reshape(seq_count, new_count, kv_count, head_dim).transpose(0, 2, 1, 3)
    fresh_values = new_values.astype(jnp.float32).reshape(seq_count, new_count, kv_count, head_dim).transpose(0, 2, 1, 3)
    cache_scores = jnp.einsum('skrd,skdl->skrl', query_block, key_cache.astype(jnp.float32)) * scale
    in_cache = jnp.arange(length)[None, :] < cache_lengths[:, None]
    cache_scores = jnp.where(in_cache[:, None, None, :], cache_scores, -1e+30)
    fresh_scores = jnp.einsum('skrd,sknd->skrn', query_block, fresh_keys) * scale
    causal = (jnp.arange(row_count) // group_size)[:, None] >= jnp.arange(new_count)[None, :]
    fresh_scores = jnp.where(causal[None, None, :, :], fresh_scores, -1e+30)
    row_max = jnp.maximum(lax.optimization_barrier(jnp.max(cache_scores, -1, keepdims=True)), lax.optimization_barrier(jnp.max(fresh_scores, -1, keepdims=True)))
    cache_exp = jnp.exp(cache_scores - row_max)
    fresh_exp = jnp.exp(fresh_scores - row_max)
    denom_sum = lax.optimization_barrier(jnp.sum(cache_exp, -1, keepdims=True)) + lax.optimization_barrier(jnp.sum(fresh_exp, -1, keepdims=True))
    cache_probs = (cache_exp / denom_sum).astype(jnp.bfloat16).astype(jnp.float32)
    fresh_probs = (fresh_exp / denom_sum).astype(jnp.bfloat16).astype(jnp.float32)
    head_mix = jnp.einsum('skrl,skdl->skrd', cache_probs, value_cache.astype(jnp.float32))
    head_mix = head_mix + jnp.einsum('skrn,sknd->skrd', fresh_probs, fresh_values)
    head_mix = head_mix.reshape(seq_count, kv_count, new_count, group_size, head_dim).transpose(0, 2, 1, 3, 4)
    return head_mix.reshape(seq_count * new_count, kv_count * group_size * head_dim).astype(jnp.bfloat16)

def expert_rows(pieces):
    buffer_rows, gate_weight, up_weight, down_weight = pieces
    gate_proj = jnp.dot(buffer_rows, gate_weight, preferred_element_type=jnp.float32)
    up_proj = jnp.dot(buffer_rows, up_weight, preferred_element_type=jnp.float32)
    activated = ((up_proj + 1.0) * gate_proj * jax.nn.sigmoid(1.702 * gate_proj)).astype(jnp.bfloat16)
    return jnp.dot(activated, down_weight, preferred_element_type=jnp.float32)

def reference(hidden, queries, new_keys, new_values, key_cache, value_cache, cache_lengths, w_out, w_router, routes, w_gate, w_up, w_down):
    blocks = (queries.reshape(N_EP, TOK_EP, HEADS * HEAD_DIM), new_keys.reshape(N_EP, TOK_EP, KV_HEADS * HEAD_DIM), new_values.reshape(N_EP, TOK_EP, KV_HEADS * HEAD_DIM), key_cache.reshape(N_EP, SEQ_DEV, KV_HEADS, HEAD_DIM, LEN), value_cache.reshape(N_EP, SEQ_DEV, KV_HEADS, HEAD_DIM, LEN), cache_lengths.reshape(N_EP, SEQ_DEV))
    attended = lax.map(lambda pieces: attend_block(*pieces), blocks).reshape(TOKENS, HEADS * HEAD_DIM)
    residual = hidden.astype(jnp.float32) + jnp.dot(attended, w_out, preferred_element_type=jnp.float32)
    normed = (residual * lax.rsqrt(lax.optimization_barrier(jnp.mean(residual * residual, -1, keepdims=True)) + 1e-05)).astype(jnp.bfloat16)
    logits = jnp.dot(normed, w_router, preferred_element_type=jnp.float32)
    picked = jnp.take_along_axis(logits, routes, 1)
    picked_exp = jnp.exp(picked)
    weights = picked_exp / lax.optimization_barrier(jnp.sum(picked_exp, -1, keepdims=True))
    flat_routes = routes.reshape(-1).astype(jnp.int32)
    one_hot = (flat_routes[:, None] == jnp.arange(EXPERTS, dtype=jnp.int32)[None, :]).astype(jnp.int32)
    slot_rank = lax.optimization_barrier(jnp.sum((jnp.cumsum(one_hot, 0) - one_hot) * one_hot, 1)).astype(jnp.int32)
    capacity = N_EP * N_TP * CAP
    buffer = jnp.zeros((EXPERTS, capacity, D), jnp.bfloat16)
    buffer = buffer.at[flat_routes, slot_rank].set(jnp.repeat(normed, TOP, axis=0))
    outputs = lax.map(expert_rows, (buffer, w_gate, w_up, w_down))
    routed = outputs[flat_routes, slot_rank].reshape(TOKENS, TOP, D)
    mixture = lax.optimization_barrier(jnp.sum(weights[:, :, None] * routed, 1))
    return (residual + mixture).astype(jnp.bfloat16)
```

```python
import jax
import jax.numpy as jnp
from jax import lax
from jax.experimental import pallas as pl
from jax.experimental.pallas import tpu as pltpu
from jax.sharding import PartitionSpec as P

MESH = pl.DeviceIdType.MESH
NZ, NX, NC, NY = 8, 4, 2, 4
NXC = NX * NC
D = 2880
FF = 384
ROWS = 16
SLOTS = 128
WIDTHS = (512, 512, 512, 512, 512, 320)
STARTS = tuple(sum(WIDTHS[:i]) for i in range(len(WIDTHS)))
C = len(WIDTHS)
BF = jnp.bfloat16
F32 = jnp.float32


def attend(queries, new_keys, new_values, key_cache, value_cache, cache_lengths):
    seq_count, kv_count, head_dim, length = key_cache.shape
    new_count = queries.shape[0] // seq_count
    group_size = queries.shape[1] // (kv_count * head_dim)
    row_count = new_count * group_size
    scale = head_dim ** (-0.5)
    query_block = queries.reshape(seq_count, new_count, kv_count, group_size, head_dim)
    query_block = query_block.transpose(0, 2, 1, 3, 4).reshape(
        seq_count, kv_count, row_count, head_dim
    )
    fresh_keys = new_keys.reshape(seq_count, new_count, kv_count, head_dim).transpose(0, 2, 1, 3)
    fresh_values = new_values.reshape(seq_count, new_count, kv_count, head_dim).transpose(
        0, 2, 1, 3
    )
    cache_scores = (
        jnp.einsum("skrd,skdl->skrl", query_block, key_cache, preferred_element_type=jnp.float32)
        * scale
    )
    in_cache = jnp.arange(length)[None, :] < cache_lengths[:, None]
    cache_scores = jnp.where(in_cache[:, None, None, :], cache_scores, -1e30)
    fresh_scores = (
        jnp.einsum("skrd,sknd->skrn", query_block, fresh_keys, preferred_element_type=jnp.float32)
        * scale
    )
    causal = (jnp.arange(row_count) // group_size)[:, None] >= jnp.arange(new_count)[None, :]
    fresh_scores = jnp.where(causal[None, None, :, :], fresh_scores, -1e30)
    row_max = jnp.maximum(
        jnp.max(cache_scores, -1, keepdims=True), jnp.max(fresh_scores, -1, keepdims=True)
    )
    cache_exp = jnp.exp(cache_scores - row_max)
    fresh_exp = jnp.exp(fresh_scores - row_max)
    denom_sum = jnp.sum(cache_exp, -1, keepdims=True) + jnp.sum(fresh_exp, -1, keepdims=True)
    cache_probs = (cache_exp / denom_sum).astype(jnp.bfloat16)
    fresh_probs = (fresh_exp / denom_sum).astype(jnp.bfloat16)
    head_mix = jnp.einsum(
        "skrl,skdl->skrd", cache_probs, value_cache, preferred_element_type=jnp.float32
    )
    head_mix = head_mix + jnp.einsum(
        "skrn,sknd->skrd", fresh_probs, fresh_values, preferred_element_type=jnp.float32
    )
    head_mix = head_mix.reshape(seq_count, kv_count, new_count, group_size, head_dim).transpose(
        0, 2, 1, 3, 4
    )
    return head_mix.reshape(seq_count * new_count, kv_count * group_size * head_dim).astype(
        jnp.bfloat16
    )


def moe_kernel(
    part, hid, routes, wr_h, wg_h, wu_h, wd_h, out,
    wr, wgu, wd, r0, res, zs, zr, xs, xa, acc, act, po, ra, rb, xs2, xr2, zs2, zr2,
    w_sem, s0s, s0r, zss, zsr, xss, xsr, yss, ysr, ras, rar, rbs, rbr, x2s, x2r, z2s, z2r,
):
    ep = lax.axis_index("ep")
    y = lax.axis_index("tp")
    c = ep % NC
    x = (ep // NC) % NX
    z = ep // NXC
    xc = x * NC + c

    wcp = [
        pltpu.make_async_copy(wr_h, wr, w_sem.at[0]),
        pltpu.make_async_copy(wg_h.at[0], wgu.at[:, pl.ds(0, FF)], w_sem.at[1]),
        pltpu.make_async_copy(wu_h.at[0], wgu.at[:, pl.ds(FF, FF)], w_sem.at[2]),
        pltpu.make_async_copy(wd_h.at[0], wd, w_sem.at[3]),
    ]
    for cp in wcp:
        cp.start()

    def zdev(j):
        return (((z + j) % NZ) * NXC + xc, y)

    def xidx(jx, jc):
        return ((x + jx) % NX) * NC + (c + jc) % NC

    def xdev(jx, jc):
        return (z * NXC + xidx(jx, jc), y)

    def ydev(d):
        return (ep, (y + d) % NY)

    XJ = [(i // NC, i % NC) for i in range(1, NXC)]

    barrier = pltpu.get_barrier_semaphore()
    peers = [zdev(j) for j in range(1, NZ)] + [xdev(*j) for j in XJ] + [ydev(d) for d in range(1, NY)]
    for dev in peers:
        pl.semaphore_signal(barrier, inc=1, device_id=dev, device_id_type=MESH)
    pl.semaphore_wait(barrier, len(peers))

    def rcopy(src, dst, ssem, rsem, dev):
        cp = pltpu.make_async_remote_copy(
            src_ref=src, dst_ref=dst, send_sem=ssem, recv_sem=rsem,
            device_id=dev, device_id_type=MESH,
        )
        cp.start()
        return cp

    started = []

    c0 = [
        rcopy(part.at[(y + d) % NY], r0.at[d - 1], s0s.at[d - 1], s0r.at[d - 1], ydev(d))
        for d in range(1, NY)
    ]
    started += c0

    rt = routes[y]
    lane = lax.broadcasted_iota(jnp.int32, (ROWS, SLOTS), 1)
    lane_e = lane // 2
    member = jnp.zeros((ROWS, SLOTS), F32)
    for r in range(4):
        member = member + jnp.where(rt[:, r : r + 1] == lane_e, 1.0, 0.0)
    ti = lax.broadcasted_iota(jnp.int32, (ROWS, ROWS), 0)
    tj = lax.broadcasted_iota(jnp.int32, (ROWS, ROWS), 1)
    lower = jnp.where(tj < ti, 1.0, 0.0).astype(BF)
    rank = jnp.dot(lower, member.astype(BF), preferred_element_type=F32)
    here = (member > 0.5) & (jnp.abs(rank - (lane % 2).astype(F32)) < 0.5)
    one_hot = jnp.where(here, 1.0, 0.0)
    pick = one_hot.T.astype(BF)

    pr = lax.broadcasted_iota(jnp.int32, (SLOTS, SLOTS), 0)
    pc = lax.broadcasted_iota(jnp.int32, (SLOTS, SLOTS), 1)
    to_x = jnp.where(pc == ((pr // 2) % 8) * 16 + (pr // 16) * 2 + pr % 2, 1.0, 0.0).astype(BF)

    for cp in c0:
        cp.wait_recv()
    resid = hid[y].astype(F32) + (
        part[y].astype(F32) + r0[0].astype(F32) + r0[1].astype(F32) + r0[2].astype(F32)
    )
    res[...] = resid
    normed = (
        resid * lax.rsqrt(jnp.mean(resid * resid, -1, keepdims=True) + 1e-05)
    ).astype(BF)

    cz = []
    for k in range(C):
        w = WIDTHS[k]
        rows = jnp.dot(pick, normed[:, STARTS[k] : STARTS[k] + w], preferred_element_type=F32)
        zs[k][...] = rows.astype(BF).reshape(NZ, ROWS, w)
        cz.append([
            rcopy(zs[k].at[(z + j) % NZ], zr[k].at[j], zss.at[k, j - 1], zsr.at[k, j - 1], zdev(j))
            for j in range(1, NZ)
        ])
        started += cz[k]
        zr[k][0] = zs[k][z]

    wcp[0].wait()
    logits = jnp.dot(normed, wr[...], preferred_element_type=F32)
    le = lax.broadcasted_iota(jnp.int32, (64, SLOTS), 0)
    ls = lax.broadcasted_iota(jnp.int32, (64, SLOTS), 1)
    spread = jnp.where(le == ls // 2, 1.0, 0.0)
    logits = jnp.dot(logits, spread, preferred_element_type=F32, precision=lax.Precision.HIGHEST)
    picked = jnp.where(here, jnp.exp(logits), 0.0)
    weight = picked / jnp.sum(picked, -1, keepdims=True)
    w_hi = weight.astype(BF)
    w_lo = (weight - w_hi.astype(F32)).astype(BF)

    wcp[1].wait()
    wcp[2].wait()
    wcp[3].wait()

    cx, cy, cf = [None] * C, [None] * C, [None] * C

    def stage_x(k):
        w = WIDTHS[k]
        for cp in cz[k]:
            cp.wait_recv()
        rows = jnp.dot(to_x, zr[k][...].reshape(SLOTS, w), preferred_element_type=F32)
        xs[k][...] = rows.astype(BF).reshape(NXC, ROWS, w)
        cx[k] = [
            rcopy(
                xs[k].at[xidx(jx, jc)], xa[k].at[0, jx * NC + jc],
                xss.at[k, jx * NC + jc - 1], xsr.at[k, jx * NC + jc - 1], xdev(jx, jc),
            )
            for jx, jc in XJ
        ]
        started.extend(cx[k])
        xa[k][0, 0] = xs[k][xc]

    def stage_y(k):
        for cp in cx[k]:
            cp.wait_recv()
        cy[k] = [
            rcopy(xa[k].at[0], xa[k].at[1], yss.at[k, 0], ysr.at[k, 0], ydev(1)),
            rcopy(xa[k].at[0], xa[k].at[3], yss.at[k, 1], ysr.at[k, 1], ydev(3)),
        ]
        started.extend(cy[k])

    def stage_f(k):
        lo, hi = pl.ds(0, NXC // 2), pl.ds(NXC // 2, NXC // 2)
        cy[k][0].wait_recv()
        a = rcopy(xa[k].at[1, lo], xa[k].at[2, lo], yss.at[k, 2], ysr.at[k, 2], ydev(1))
        cy[k][1].wait_recv()
        b = rcopy(xa[k].at[3, hi], xa[k].at[2, hi], yss.at[k, 3], ysr.at[k, 3], ydev(3))
        cf[k] = [a, b]
        started.extend(cf[k])

    def stage_m(k):
        w = WIDTHS[k]
        for cp in cf[k]:
            cp.wait_recv()
        g = jnp.dot(
            xa[k][...].reshape(NY * SLOTS, w), wgu[pl.ds(STARTS[k], w), :],
            preferred_element_type=F32,
        )
        if k == 0:
            acc[...] = g
        else:
            acc[...] += g

    for k in range(C + 3):
        if k < C:
            stage_x(k)
        if 0 <= k - 1 < C:
            stage_y(k - 1)
        if 0 <= k - 2 < C:
            stage_f(k - 2)
        if 0 <= k - 3 < C:
            stage_m(k - 3)

    gate = acc[:, 0:FF]
    up = acc[:, FF : 2 * FF]
    act[...] = ((up + 1.0) * gate * jax.nn.sigmoid(1.702 * gate)).astype(BF)

    ca, cb, cx2, cz2 = [None] * C, [None] * C, [None] * C, [None] * C
    half = SLOTS // 2
    lo, hi = pl.ds(0, half), pl.ds(half, half)

    def ret_a(k):
        w = WIDTHS[k]
        p = jnp.dot(act[...], wd[:, STARTS[k] : STARTS[k] + w], preferred_element_type=F32)
        po[k][...] = p.astype(BF).reshape(NY, SLOTS, w)
        ca[k] = [
            rcopy(po[k].at[2, lo], ra[k].at[0], ras.at[k, 0], rar.at[k, 0], ydev(1)),
            rcopy(po[k].at[2, hi], ra[k].at[1], ras.at[k, 1], rar.at[k, 1], ydev(3)),
        ]
        started.extend(ca[k])

    def ret_b(k):
        ca[k][0].wait_recv()
        po[k][3, lo] = (po[k][3, lo].astype(F32) + ra[k][0].astype(F32)).astype(BF)
        a = rcopy(po[k].at[3], rb[k].at[0], rbs.at[k, 0], rbr.at[k, 0], ydev(1))
        ca[k][1].wait_recv()
        po[k][1, hi] = (po[k][1, hi].astype(F32) + ra[k][1].astype(F32)).astype(BF)
        b = rcopy(po[k].at[1], rb[k].at[1], rbs.at[k, 1], rbr.at[k, 1], ydev(3))
        cb[k] = [a, b]
        started.extend(cb[k])

    def ret_x(k):
        w = WIDTHS[k]
        for cp in cb[k]:
            cp.wait_recv()
        total = po[k][0].astype(F32) + rb[k][0].astype(F32) + rb[k][1].astype(F32)
        xs2[k][...] = total.astype(BF).reshape(NXC, ROWS, w)
        cx2[k] = [
            rcopy(
                xs2[k].at[jx * NC + jc], xr2[k].at[xc],
                x2s.at[k, jx * NC + jc - 1], x2r.at[k, jx * NC + jc - 1], xdev(NX - jx, NC - jc),
            )
            for jx, jc in XJ
        ]
        started.extend(cx2[k])
        xr2[k][xc] = xs2[k][0]

    def ret_z(k):
        w = WIDTHS[k]
        for cp in cx2[k]:
            cp.wait_recv()
        rows = jnp.dot(to_x, xr2[k][...].reshape(SLOTS, w), preferred_element_type=F32)
        zs2[k][...] = rows.astype(BF).reshape(NZ, ROWS, w)
        cz2[k] = [
            rcopy(
                zs2[k].at[j], zr2[k].at[z], z2s.at[k, j - 1], z2r.at[k, j - 1], zdev(NZ - j)
            )
            for j in range(1, NZ)
        ]
        started.extend(cz2[k])
        zr2[k][z] = zs2[k][0]

    def finish(k):
        w = WIDTHS[k]
        for cp in cz2[k]:
            cp.wait_recv()
        rows = zr2[k][...].reshape(SLOTS, w)
        mix = jnp.dot(w_hi, rows, preferred_element_type=F32) + jnp.dot(
            w_lo, rows, preferred_element_type=F32
        )
        cols = slice(STARTS[k], STARTS[k] + w)
        out[:, cols] = (res[:, cols] + mix).astype(BF)

    for k in range(C + 4):
        if k < C:
            ret_a(k)
        if 0 <= k - 1 < C:
            ret_b(k - 1)
        if 0 <= k - 2 < C:
            ret_x(k - 2)
        if 0 <= k - 3 < C:
            ret_z(k - 3)
        if 0 <= k - 4 < C:
            finish(k - 4)

    for cp in started:
        cp.wait_send()


def moe(part, hid, routes, w_router, w_gate, w_up, w_down):
    vm = pl.BlockSpec(memory_space=pltpu.VMEM)
    hbm = pl.BlockSpec(memory_space=pl.ANY)

    def bufs(*lead):
        return [pltpu.VMEM((*lead, w), BF) for w in WIDTHS]

    dma = pltpu.SemaphoreType.DMA
    return pl.pallas_call(
        moe_kernel,
        out_shape=jax.ShapeDtypeStruct((ROWS, D), BF),
        in_specs=[vm, vm, vm, hbm, hbm, hbm, hbm],
        out_specs=vm,
        scratch_shapes=[
            pltpu.VMEM((D, 64), BF),
            pltpu.VMEM((D, 2 * FF), BF),
            pltpu.VMEM((FF, D), BF),
            pltpu.VMEM((3, ROWS, D), BF),
            pltpu.VMEM((ROWS, D), F32),
            bufs(NZ, ROWS),
            bufs(NZ, ROWS),
            bufs(NXC, ROWS),
            bufs(NY, NXC, ROWS),
            pltpu.VMEM((NY * SLOTS, 2 * FF), F32),
            pltpu.VMEM((NY * SLOTS, FF), BF),
            bufs(NY, SLOTS),
            bufs(2, SLOTS // 2),
            bufs(2, SLOTS),
            bufs(NXC, ROWS),
            bufs(NXC, ROWS),
            bufs(NZ, ROWS),
            bufs(NZ, ROWS),
            dma((4,)),
            dma((3,)), dma((3,)),
            dma((C, 7)), dma((C, 7)),
            dma((C, 7)), dma((C, 7)),
            dma((C, 4)), dma((C, 4)),
            dma((C, 2)), dma((C, 2)),
            dma((C, 2)), dma((C, 2)),
            dma((C, 7)), dma((C, 7)),
            dma((C, 7)), dma((C, 7)),
        ],
        compiler_params=pltpu.CompilerParams(
            collective_id=0, has_side_effects=True, vmem_limit_bytes=56 * 1024 * 1024
        ),
    )(part, hid, routes, w_router, w_gate, w_up, w_down)


def body(
    hidden,
    queries,
    new_keys,
    new_values,
    key_cache,
    value_cache,
    cache_lengths,
    w_out,
    w_router,
    routes,
    w_gate,
    w_up,
    w_down,
):
    attended = attend(queries, new_keys, new_values, key_cache, value_cache, cache_lengths)
    part = jnp.dot(attended, w_out, preferred_element_type=jnp.float32).astype(BF)
    return moe(
        part.reshape(NY, ROWS, D),
        hidden.reshape(NY, ROWS, D),
        routes.reshape(NY, ROWS, 4),
        w_router,
        w_gate,
        w_up,
        w_down,
    )


def solution(mesh):
    return jax.shard_map(
        body,
        mesh=mesh,
        in_specs=(
            P("ep", None),
            P("ep", "tp"),
            P("ep", "tp"),
            P("ep", "tp"),
            P("ep", "tp", None, None),
            P("ep", "tp", None, None),
            P("ep"),
            P("tp", None),
            P(),
            P("ep", None),
            P("ep", None, "tp"),
            P("ep", None, "tp"),
            P("ep", "tp", None),
        ),
        out_specs=P(("ep", "tp"), None),
        check_vma=False,
    )
```

```python
import jax
import jax.numpy as jnp
from jax import lax
from jax.experimental import pallas as pl
from jax.experimental.pallas import tpu as pltpu
from jax.sharding import PartitionSpec as P

MESH = pl.DeviceIdType.MESH
NZ, NX, NC, NY = 8, 4, 2, 4
NXC = NX * NC
D = 2880
FF = 384
LEN = 1024
ROWS = 16
SLOTS = 128
K = 3
PAD = K * 1024
DP = 2944
CUT = 1536
GROUPS = ((0,), (1, 7), (3, 5), (4,), (2,), (6,))
MULS = ((0, 1), (2, 3), (4, 5))
ORDER = (
    "s0", "s1", "s2", "s3", "s4", "s5", "y0", "y1", "f0", "y2", "y3", "f2",
    "f3", "y4", "y5", "f1", "m1", "a2", "a3", "f4", "f5", "b2", "m0", "a1",
    "b3", "m2", "a4", "a5", "x2", "b1", "a0", "b4", "b5", "x3", "x1", "w0",
    "b0", "x4", "x5", "x0",
)
JZ = tuple(j for g in GROUPS for j in g)
CLASSES = tuple((sum(map(len, GROUPS[:i])), sum(map(len, GROUPS[: i + 1]))) for i in range(len(GROUPS)))
MULS = tuple((m[0], m[-1] + 1) for m in MULS)
BF = jnp.bfloat16
F32 = jnp.float32


def moe_kernel(
    lens, q_h, nk_h, nv_h, hid_h, rt_h, kc_h, vc_h, wo_h, wr_h, wg_h, wu_h, wd_h, out,
    q, nk, nv, hid, routes, sco, prb, kc, vc, wo, part, wr, wgu, wd, r0, res, nrm, zs, xa, xm, po, ra1, ra2, rb, ys, rr,
    met, in_sem, kv_sem, w_sem, s0s, s0r, zss, zsr, yss, ysr, ras, rar, rbs, rbr, xss, xsr,
):
    ep = lax.axis_index("ep")
    y = lax.axis_index("tp")
    c = ep % NC
    x = (ep // NC) % NX
    z = ep // NXC
    xc = x * NC + c

    turns = (2, 1, 3, 0)
    blocks = [(y + d) % NY for d in turns]
    kvcp = []
    for i, b in enumerate(blocks):
        two = pl.ds(b * 2, 2)
        kvcp.append((
            pltpu.make_async_copy(kc_h.at[two, 0], kc.at[i], kv_sem.at[0, i]),
            pltpu.make_async_copy(vc_h.at[two, 0], vc.at[i], kv_sem.at[1, i]),
        ))
    wocp = pltpu.make_async_copy(wo_h, wo, w_sem.at[4])
    wcp = [
        pltpu.make_async_copy(wr_h, wr, w_sem.at[0]),
        pltpu.make_async_copy(wg_h.at[0], wgu.at[:, pl.ds(0, FF)], w_sem.at[1]),
        pltpu.make_async_copy(wu_h.at[0], wgu.at[:, pl.ds(FF, FF)], w_sem.at[2]),
        pltpu.make_async_copy(wd_h.at[0], wd.at[pl.ds(0, D)], w_sem.at[3]),
    ]
    small = [(q_h, q), (nk_h, nk), (nv_h, nv), (rt_h, routes), (hid_h, hid)]
    incp = [pltpu.make_async_copy(a, b, in_sem.at[i]) for i, (a, b) in enumerate(small)]
    incp[0].start()
    for pair in kvcp[:3]:
        pair[0].start()
    for cp in incp[1:3]:
        cp.start()
    for pair in kvcp[:3]:
        pair[1].start()
    wocp.start()
    for cp in kvcp[3]:
        cp.start()
    for cp in incp[3:]:
        cp.start()

    def eidx(jz, i, sign=1):
        jx, jc = sign * (i // NC), i % NC
        return ((z + sign * jz) % NZ) * NXC + ((x + jx) % NX) * NC + (c + jc) % NC

    def ydev(d):
        return (ep, (y + d) % NY)

    FAR = (4, 5, 2, 3, 6, 7, 1, 0)
    PEERS = [(p, i) for p in range(NZ) for i in FAR if (p, i) != (0, 0)]

    barrier = pltpu.get_barrier_semaphore()
    LINES = [(eidx(j, 0), y) for j in range(1, NZ)] + [ydev(d) for d in range(1, NY)]
    CROSS = [(eidx(0, i), y) for i in FAR if i]
    for dev in LINES + CROSS:
        pl.semaphore_signal(barrier, inc=1, device_id=dev, device_id_type=MESH)

    def rcopy(src, dst, ssem, rsem, dev):
        cp = pltpu.make_async_remote_copy(
            src_ref=src, dst_ref=dst, send_sem=ssem, recv_sem=rsem,
            device_id=dev, device_id_type=MESH,
        )
        cp.start()
        return cp

    started = []

    pos = lax.broadcasted_iota(jnp.int32, (64, LEN), 1)
    causal = (
        lax.broadcasted_iota(jnp.int32, (64, 8), 0) % 8
        >= lax.broadcasted_iota(jnp.int32, (64, 8), 1)
    )
    scale = 64 ** (-0.5)

    def attend(which):
        rows = [(i, s) for i in which for s in range(2)]
        fresh, mixes = {}, []
        for i, s in rows:
            if s == 0:
                kvcp[i][0].wait()
            b = blocks[i]
            r = slice(s * 8, s * 8 + 8)
            qb, nkb = q[b].astype(F32), nk[b].astype(F32)
            qs = jnp.concatenate([qb[r, h * 64 : h * 64 + 64] for h in range(8)], 0).astype(BF)
            sc = jnp.dot(qs, kc[i, s], preferred_element_type=F32) * scale
            sco[i * 2 + s] = jnp.where(pos < lens[b * 2 + s], sc, -1e30)
            fs = lax.dot_general(
                qs, nkb[r].astype(BF), (((1,), (1,)), ((), ())), preferred_element_type=F32
            ) * scale
            fresh[i, s] = jnp.where(causal, fs, -1e30)
        for i, s in rows:
            sc, fs = sco[i * 2 + s], fresh[i, s]
            top = jnp.maximum(jnp.max(sc, -1, keepdims=True), jnp.max(fs, -1, keepdims=True))
            se = jnp.exp(sc - top)
            fe = jnp.exp(fs - top)
            inv = 1.0 / (jnp.sum(se, -1, keepdims=True) + jnp.sum(fe, -1, keepdims=True))
            prb[i * 2 + s] = (se * inv).astype(BF)
            fresh[i, s] = (fe * inv).astype(BF)
        for i, s in rows:
            if s == 0:
                kvcp[i][1].wait()
            r = slice(s * 8, s * 8 + 8)
            nvb = nv[blocks[i]].astype(F32)
            mix = lax.dot_general(
                prb[i * 2 + s], vc[i, s], (((1,), (1,)), ((), ())), preferred_element_type=F32
            ) + jnp.dot(fresh[i, s], nvb[r].astype(BF), preferred_element_type=F32)
            mixes.append(jnp.concatenate([mix[h * 8 : h * 8 + 8] for h in range(8)], 1))
        return jnp.concatenate(mixes, 0).astype(BF)

    def project(att):
        return lax.dot_general(
            att, wo[...], (((1,), (1,)), ((), ())), preferred_element_type=F32
        ).astype(BF)

    c0 = []

    def send_part(d):
        c0.append(
            rcopy(part.at[d], r0.at[d - 1], s0s.at[d - 1], s0r.at[d - 1], ydev(d))
        )

    with jax.named_scope("in0"):
        for cp in incp[:3]:
            cp.wait()
    with jax.named_scope("at0"):
        att = attend((0, 1, 2))
        for cp in wcp:
            cp.start()
    with jax.named_scope("wo0"):
        wocp.wait()
        three = project(att)
        for i in range(3):
            part[turns[i]] = three[i * ROWS : (i + 1) * ROWS]
    with jax.named_scope("bar"):
        pl.semaphore_wait(barrier, len(LINES) + len(CROSS))
        for dev in CROSS:
            pl.semaphore_signal(met, inc=1, device_id=dev, device_id_type=MESH)
        for d in turns[:3]:
            send_part(d)
        started += c0
    with jax.named_scope("at2"):
        att = attend((3,))
        for cp in incp[3:]:
            cp.wait()
    with jax.named_scope("wo2"):
        part[0] = project(att)

    own_r = lax.broadcasted_iota(jnp.int32, (ROWS, NY * ROWS), 0) + y * ROWS
    own_c = lax.broadcasted_iota(jnp.int32, (ROWS, NY * ROWS), 1)
    own = jnp.where(own_r == own_c, 1.0, 0.0).astype(BF)
    rt = lax.dot_general(
        own, routes[...].astype(F32).astype(BF), (((1,), (1,)), ((), ())),
        preferred_element_type=F32,
    )
    lane = lax.broadcasted_iota(jnp.int32, (ROWS, SLOTS), 1)
    lane_f = (lane // 2).astype(F32)
    member = jnp.zeros((ROWS, SLOTS), F32)
    for r in range(4):
        member = member + jnp.where(rt[:, r : r + 1] == lane_f, 1.0, 0.0)
    ti = lax.broadcasted_iota(jnp.int32, (ROWS, ROWS), 0)
    tj = lax.broadcasted_iota(jnp.int32, (ROWS, ROWS), 1)
    lower = jnp.where(tj < ti, 1.0, 0.0).astype(BF)
    rank = jnp.dot(lower, member.astype(BF), preferred_element_type=F32)
    here = (member > 0.5) & (jnp.abs(rank - (lane % 2).astype(F32)) < 0.5)
    one_hot = jnp.where(here, 1.0, 0.0)

    er = lax.broadcasted_iota(jnp.int32, (SLOTS, 1024), 0)
    ec = lax.broadcasted_iota(jnp.int32, (SLOTS, 1024), 1)
    expand = jnp.where(er == (ec // 16) * 2 + ec % 2, 1.0, 0.0).astype(BF)
    same_g = er // ROWS == (ec // 2) % 8

    def spread_out(v):
        wide = jnp.dot(v, expand, preferred_element_type=F32)
        return jnp.where(same_g, jnp.concatenate([wide] * 8, 0), 0.0)

    pick = spread_out(one_hot.astype(BF)).T.astype(BF)

    pr = lax.broadcasted_iota(jnp.int32, (SLOTS, SLOTS), 0)
    pc = lax.broadcasted_iota(jnp.int32, (SLOTS, SLOTS), 1)
    swap = jnp.where(pc == ((pr // 2) % 8) * 16 + (pr // 16) * 2 + pr % 2, 1.0, 0.0).astype(BF)
    wd[pl.ds(D, DP - D)] = jnp.zeros((DP - D, FF), BF)

    with jax.named_scope("w0"):
        for cp in c0:
            cp.wait_recv()
    resid = hid[y].astype(F32) + (
        part[0].astype(F32) + r0[0].astype(F32) + r0[1].astype(F32) + r0[2].astype(F32)
    )
    res[...] = resid
    normed = (
        resid * lax.rsqrt(jnp.mean(resid * resid, -1, keepdims=True) + 1e-05)
    ).astype(BF)

    nrm[...] = jnp.concatenate([normed, jnp.zeros((ROWS, PAD - D), BF)], 1)
    for k in range(K):
        tok = jnp.concatenate(
            [nrm[:, k * 1024 + g * 128 : k * 1024 + g * 128 + 128] for g in range(8)], 0
        )
        rows = jnp.dot(pick, tok, preferred_element_type=F32)
        zs[:, k] = rows.astype(BF).reshape(64, ROWS, 128)
    pl.semaphore_wait(met, len(CROSS))
    xa[0, 0, 0] = zs[ep]

    def stage_s(n):
        for p, i in PEERS:
            if CLASSES[n][0] <= p < CLASSES[n][1]:
                e = eidx(JZ[p], i)
                rcopy(zs.at[e], xa.at[0, p, i], zss.at[0], zsr.at[p], (e, y))

    def arrived(sem, n):
        pltpu.make_async_remote_copy(
            src_ref=zs.at[pl.ds(0, n)], dst_ref=rr.at[pl.ds(0, n)], send_sem=zss.at[0],
            recv_sem=sem, device_id=(ep, (y + 1) % NY), device_id_type=MESH,
        ).wait_recv()

    def sent(sem, n):
        pltpu.make_async_remote_copy(
            src_ref=zs.at[pl.ds(0, n)], dst_ref=rr.at[pl.ds(0, n)], send_sem=sem,
            recv_sem=zsr.at[0], device_id=(ep, (y + 1) % NY), device_id_type=MESH,
        ).wait_send()

    def group(p):
        return NXC - 1 if p == 0 else NXC

    late = {}

    def weigh(_):
        wcp[0].wait()
        logits = lax.dot_general(
            nrm[:, 0:D], wr[...], (((1,), (1,)), ((), ())), preferred_element_type=F32
        )
        le = lax.broadcasted_iota(jnp.int32, (64, SLOTS), 0)
        ls = lax.broadcasted_iota(jnp.int32, (64, SLOTS), 1)
        spread = jnp.where(le == ls // 2, 1.0, 0.0)
        logits = jnp.dot(
            logits, spread, preferred_element_type=F32, precision=lax.Precision.HIGHEST
        )
        picked = jnp.where(here, jnp.exp(logits), 0.0)
        weight = picked / jnp.sum(picked, -1, keepdims=True)
        hi = weight.astype(BF)
        late["hi"] = spread_out(hi).astype(BF)
        late["lo"] = spread_out((weight - hi.astype(F32)).astype(BF)).astype(BF)

    cy, cf, ca, cb = {}, {}, {}, {}

    def stage_y(i):
        p0, p1 = CLASSES[i]
        ps = pl.ds(p0, p1 - p0)
        for p in range(p0, p1):
            arrived(zsr.at[p], group(p))
        cy[i] = [
            rcopy(xa.at[0, ps], xa.at[1, ps], yss.at[i, 0], ysr.at[i, 0], ydev(1)),
            rcopy(xa.at[0, ps], xa.at[3, ps], yss.at[i, 1], ysr.at[i, 1], ydev(3)),
        ]
        started.extend(cy[i])

    def stage_f(i):
        p0, p1 = CLASSES[i]
        ps = pl.ds(p0, p1 - p0)
        lo, hi = pl.ds(0, NXC // 2), pl.ds(NXC // 2, NXC // 2)
        cy[i][0].wait_recv()
        a = rcopy(xa.at[1, ps, lo], xa.at[2, ps, lo], yss.at[i, 2], ysr.at[i, 2], ydev(1))
        cy[i][1].wait_recv()
        b = rcopy(xa.at[3, ps, hi], xa.at[2, ps, hi], yss.at[i, 3], ysr.at[i, 3], ydev(3))
        cf[i] = [a, b]
        started.extend(cf[i])

    def stage_m(i):
        i0, i1 = MULS[i]
        p0, p1 = CLASSES[i0][0], CLASSES[i1 - 1][1]
        n = p1 - p0
        for j in range(i0, i1):
            for cp in cf[j]:
                cp.wait_recv()
        while len(wcp) > 1:
            wcp.pop().wait()

        def unfold(d, _):
            for q in range(n):
                blk = jnp.concatenate(
                    [xa[d, p0 + q, :, k].reshape(SLOTS, 128) for k in range(K)], 1
                )
                r = jnp.dot(swap, blk, preferred_element_type=F32).astype(BF)
                for k in range(K):
                    for g in range(8):
                        xm[d, q, :, k * 1024 + g * 128 : k * 1024 + g * 128 + 128] = r[
                            g * ROWS : (g + 1) * ROWS, k * 128 : k * 128 + 128
                        ]
            return 0

        lax.fori_loop(0, NY, unfold, 0)
        rows = xm[:, 0:n, :, 0:D].reshape(NY * n * ROWS, D)
        h = jnp.dot(rows, wgu[...], preferred_element_type=F32)
        gate, up = h[:, 0:FF], h[:, FF : 2 * FF]
        act = ((up + 1.0) * gate * jax.nn.sigmoid(1.702 * gate)).astype(BF)
        o = lax.dot_general(act, wd[...], (((1,), (1,)), ((), ())), preferred_element_type=F32)
        po[:, p0:p1] = o.astype(BF).reshape(NY, n, ROWS, DP)

    lo, hi = pl.ds(0, CUT), pl.ds(CUT, DP - CUT)

    def ret_a(i):
        p0, p1 = CLASSES[i]
        ps = pl.ds(p0, p1 - p0)
        ca[i] = [
            rcopy(po.at[2, ps, :, lo], ra1.at[ps], ras.at[i, 0], rar.at[i, 0], ydev(1)),
            rcopy(po.at[2, ps, :, hi], ra2.at[ps], ras.at[i, 1], rar.at[i, 1], ydev(3)),
        ]
        started.extend(ca[i])

    def ret_b(i):
        p0, p1 = CLASSES[i]
        ps = pl.ds(p0, p1 - p0)
        ca[i][0].wait_recv()
        po[3, ps, :, lo] = (po[3, ps, :, lo].astype(F32) + ra1[ps].astype(F32)).astype(BF)
        a = rcopy(po.at[3, ps], rb.at[0, ps], rbs.at[i, 0], rbr.at[i, 0], ydev(1))
        ca[i][1].wait_recv()
        po[1, ps, :, hi] = (po[1, ps, :, hi].astype(F32) + ra2[ps].astype(F32)).astype(BF)
        b = rcopy(po.at[1, ps], rb.at[1, ps], rbs.at[i, 1], rbr.at[i, 1], ydev(3))
        cb[i] = [a, b]
        started.extend(cb[i])

    def ret_x(i):
        p0, p1 = CLASSES[i]
        for cp in cb[i]:
            cp.wait_recv()
        for p in range(p0, p1):
            tot = (
                po[0, p].astype(F32) + rb[0, p].astype(F32) + rb[1, p].astype(F32)
            ).astype(BF)
            tot = jnp.concatenate([tot, jnp.zeros((ROWS, PAD - DP), BF)], 1)
            blk = jnp.concatenate(
                [
                    jnp.concatenate(
                        [tot[:, k * 1024 + g * 128 : k * 1024 + g * 128 + 128] for g in range(8)], 0
                    )
                    for k in range(K)
                ],
                1,
            )
            r = jnp.dot(swap, blk, preferred_element_type=F32).astype(BF)
            for k in range(K):
                ys[p, :, k] = r[:, k * 128 : k * 128 + 128].reshape(NXC, ROWS, 128)
            for j in FAR:
                if (p, j) != (0, 0):
                    rcopy(
                        ys.at[p, j], rr.at[ep], xss.at[0], xsr.at[p],
                        (eidx(JZ[p], j, -1), y),
                    )
        if p0 == 0:
            rr[ep] = ys[0, 0]

    steps = {"s": stage_s, "y": stage_y, "f": stage_f, "m": stage_m, "w": weigh, "a": ret_a, "b": ret_b, "x": ret_x}
    for step in ORDER:
        with jax.named_scope(f"d{step}"):
            steps[step[0]](int(step[1]))

    with jax.named_scope("wr"):
        for p in range(NZ):
            arrived(xsr.at[p], group(p))
    for k in range(K):
        rows = rr[:, k].reshape(1024, 128)
        mix = jnp.dot(late["hi"], rows, preferred_element_type=F32) + jnp.dot(
            late["lo"], rows, preferred_element_type=F32
        )
        for g in range(8):
            c0_ = k * 1024 + g * 128
            c1_ = min(c0_ + 128, D)
            if c1_ > c0_:
                out[:, c0_:c1_] = (
                    res[:, c0_:c1_] + mix[g * ROWS : (g + 1) * ROWS, 0 : c1_ - c0_]
                )

    sent(zss.at[0], NZ * NXC - 1)
    sent(xss.at[0], NZ * NXC - 1)
    for cp in started:
        cp.wait_send()


def moe(*args):
    vm = pl.BlockSpec(memory_space=pltpu.VMEM)
    hbm = pl.BlockSpec(memory_space=pl.ANY)

    n = len(CLASSES)
    dma = pltpu.SemaphoreType.DMA
    return pl.pallas_call(
        moe_kernel,
        out_shape=jax.ShapeDtypeStruct((ROWS, D), F32),
        in_specs=[pl.BlockSpec(memory_space=pltpu.SMEM)] + [hbm] * 12,
        out_specs=vm,
        scratch_shapes=[
            pltpu.VMEM((NY, ROWS, 512), BF),
            pltpu.VMEM((NY, ROWS, 64), BF),
            pltpu.VMEM((NY, ROWS, 64), BF),
            pltpu.VMEM((NY, ROWS, D), BF),
            pltpu.VMEM((4, NY * ROWS), jnp.int32),
            pltpu.VMEM((8, 64, LEN), F32),
            pltpu.VMEM((8, 64, LEN), BF),
            pltpu.VMEM((NY, 2, 64, LEN), BF),
            pltpu.VMEM((NY, 2, 64, LEN), BF),
            pltpu.VMEM((D, 512), BF),
            pltpu.VMEM((NY, ROWS, D), BF),
            pltpu.VMEM((64, D), BF),
            pltpu.VMEM((D, 2 * FF), BF),
            pltpu.VMEM((DP, FF), BF),
            pltpu.VMEM((3, ROWS, D), BF),
            pltpu.VMEM((ROWS, D), F32),
            pltpu.VMEM((ROWS, PAD), BF),
            pltpu.VMEM((NZ * NXC, K, ROWS, 128), BF),
            pltpu.VMEM((NY, NZ, NXC, K, ROWS, 128), BF),
            pltpu.VMEM((NY, 3, ROWS, PAD), BF),
            pltpu.VMEM((NY, NZ, ROWS, DP), BF),
            pltpu.VMEM((NZ, ROWS, CUT), BF),
            pltpu.VMEM((NZ, ROWS, DP - CUT), BF),
            pltpu.VMEM((2, NZ, ROWS, DP), BF),
            pltpu.VMEM((NZ, NXC, K, ROWS, 128), BF),
            pltpu.VMEM((NZ * NXC, K, ROWS, 128), BF),
            pltpu.SemaphoreType.REGULAR,
            dma((5,)),
            dma((2, NY)),
            dma((5,)),
            dma((3,)), dma((3,)),
            dma((1,)), dma((NZ,)),
            dma((n, 4)), dma((n, 4)),
            dma((n, 2)), dma((n, 2)),
            dma((n, 2)), dma((n, 2)),
            dma((1,)), dma((NZ,)),
        ],
        compiler_params=pltpu.CompilerParams(
            collective_id=0, has_side_effects=True, vmem_limit_bytes=56 * 1024 * 1024
        ),
    )(*args)


def body(
    hidden,
    queries,
    new_keys,
    new_values,
    key_cache,
    value_cache,
    cache_lengths,
    w_out,
    w_router,
    routes,
    w_gate,
    w_up,
    w_down,
):
    return moe(
        cache_lengths,
        queries.reshape(NY, ROWS, 512),
        new_keys.reshape(NY, ROWS, 64),
        new_values.reshape(NY, ROWS, 64),
        hidden.reshape(NY, ROWS, D),
        routes.T,
        key_cache,
        value_cache,
        w_out.T,
        w_router.T,
        w_gate,
        w_up,
        w_down.transpose(0, 2, 1),
    ).astype(BF)


def solution(mesh):
    return jax.shard_map(
        body,
        mesh=mesh,
        in_specs=(
            P("ep", None),
            P("ep", "tp"),
            P("ep", "tp"),
            P("ep", "tp"),
            P("ep", "tp", None, None),
            P("ep", "tp", None, None),
            P("ep"),
            P("tp", None),
            P(),
            P("ep", None),
            P("ep", None, "tp"),
            P("ep", None, "tp"),
            P("ep", "tp", None),
        ),
        out_specs=P(("ep", "tp"), None),
        check_vma=False,
    )
```

```python
import jax
import jax.numpy as jnp
from jax import lax
from jax.experimental import pallas as pl
from jax.experimental.pallas import tpu as pltpu
from jax.sharding import PartitionSpec as P

MESH = pl.DeviceIdType.MESH
NZ, NX, NC, NY = 8, 4, 2, 4
NXC = NX * NC
D = 2880
FF = 384
LEN = 1024
ROWS = 16
SLOTS = 128
K = 3
PAD = K * 1024
DP = 2944
CUT = 1536
GROUPS = ((0,), (1,), (7,), (3,), (5,), (4,), (2,), (6,))
MULS = ((0, 1, 2), (3, 4), (5, 6, 7))
ORDER = (
    "s4", "s3", "s0", "y0", "s6", "s1", "y4", "s7", "f0", "s5", "y3", "f4",
    "s2", "y6", "w0", "y1", "f3", "y7", "f6", "y5", "y2", "m1", "a3", "f7",
    "f5", "a4", "f1", "f2", "b3", "m2", "a6", "a5", "b4", "m0", "a2", "a7",
    "x3", "b5", "b6", "x4", "a1", "b2", "a0", "x5", "b7", "b1", "x6", "b0",
    "x2", "x7", "x1", "x0",
)
JZ = tuple(j for g in GROUPS for j in g)
CLASSES = tuple((sum(map(len, GROUPS[:i])), sum(map(len, GROUPS[: i + 1]))) for i in range(len(GROUPS)))
MULS = tuple((m[0], m[-1] + 1) for m in MULS)
BF = jnp.bfloat16
F32 = jnp.float32


def moe_kernel(
    lens, q_h, nk_h, nv_h, hid_h, rt_h, kc_h, vc_h, wo_h, wr_h, wg_h, wu_h, wd_h, out,
    q, nk, nv, hid, routes, sco, prb, kc, vc, wo, part, wr, wgu, wd, r0, res, nrm, zs, xr, xn, po, ra1, ra2, rb, ys, rr,
    met, in_sem, kv_sem, w_sem, s0s, s0r, zss, zsr, yss, ysr, ras, rar, rbs, rbr, xss, xsr,
):
    ep = lax.axis_index("ep")
    y = lax.axis_index("tp")
    c = ep % NC
    x = (ep // NC) % NX
    z = ep // NXC
    xc = x * NC + c

    turns = (2, 1, 3, 0)
    blocks = [(y + d) % NY for d in turns]
    kvcp = []
    for i, b in enumerate(blocks):
        two = pl.ds(b * 2, 2)
        kvcp.append((
            pltpu.make_async_copy(kc_h.at[two, 0], kc.at[i], kv_sem.at[0, i]),
            pltpu.make_async_copy(vc_h.at[two, 0], vc.at[i], kv_sem.at[1, i]),
        ))
    wocp = pltpu.make_async_copy(wo_h, wo.at[pl.ds(0, D)], w_sem.at[4])
    wcp = [
        pltpu.make_async_copy(wr_h, wr, w_sem.at[0]),
        pltpu.make_async_copy(wg_h.at[0], wgu.at[:, pl.ds(0, FF)], w_sem.at[1]),
        pltpu.make_async_copy(wu_h.at[0], wgu.at[:, pl.ds(FF, FF)], w_sem.at[2]),
        pltpu.make_async_copy(wd_h.at[0], wd.at[pl.ds(0, D)], w_sem.at[3]),
    ]
    small = [(q_h, q), (nk_h, nk), (nv_h, nv), (rt_h, routes), (hid_h, hid)]
    incp = [pltpu.make_async_copy(a, b, in_sem.at[i]) for i, (a, b) in enumerate(small)]
    incp[0].start()
    for pair in kvcp[:3]:
        pair[0].start()
    for cp in incp[1:3]:
        cp.start()
    for pair in kvcp[:3]:
        pair[1].start()
    wocp.start()
    for cp in kvcp[3]:
        cp.start()
    for cp in incp[3:]:
        cp.start()

    def eidx(jz, i, sign=1):
        jx, jc = sign * (i // NC), i % NC
        return ((z + sign * jz) % NZ) * NXC + ((x + jx) % NX) * NC + (c + jc) % NC

    def ydev(d):
        return (ep, (y + d) % NY)

    FAR = (4, 5, 2, 3, 6, 7, 1, 0)
    PEERS = [(p, i) for p in range(NZ) for i in FAR if (p, i) != (0, 0)]

    barrier = pltpu.get_barrier_semaphore()
    LINES = [(eidx(j, 0), y) for j in range(1, NZ)] + [ydev(d) for d in range(1, NY)]
    CROSS = [(eidx(0, i), y) for i in FAR if i]
    for dev in LINES + CROSS:
        pl.semaphore_signal(barrier, inc=1, device_id=dev, device_id_type=MESH)

    def rcopy(src, dst, ssem, rsem, dev):
        cp = pltpu.make_async_remote_copy(
            src_ref=src, dst_ref=dst, send_sem=ssem, recv_sem=rsem,
            device_id=dev, device_id_type=MESH,
        )
        cp.start()
        return cp

    started = []

    pos = lax.broadcasted_iota(jnp.int32, (64, LEN), 1)
    causal = (
        lax.broadcasted_iota(jnp.int32, (64, 8), 0) % 8
        >= lax.broadcasted_iota(jnp.int32, (64, 8), 1)
    )
    scale = 64 ** (-0.5)

    def attend(which):
        rows = [(i, s) for i in which for s in range(2)]
        fresh, mixes = {}, []
        for i, s in rows:
            if s == 0:
                kvcp[i][0].wait()
            b = blocks[i]
            r = slice(s * 8, s * 8 + 8)
            qb, nkb = q[b].astype(F32), nk[b].astype(F32)
            qs = jnp.concatenate([qb[r, h * 64 : h * 64 + 64] for h in range(8)], 0).astype(BF)
            sc = jnp.dot(qs, kc[i, s], preferred_element_type=F32) * scale
            sco[i * 2 + s] = jnp.where(pos < lens[b * 2 + s], sc, -1e30)
            fs = lax.dot_general(
                qs, nkb[r].astype(BF), (((1,), (1,)), ((), ())), preferred_element_type=F32
            ) * scale
            fresh[i, s] = jnp.where(causal, fs, -1e30)
        for i, s in rows:
            sc, fs = sco[i * 2 + s], fresh[i, s]
            top = jnp.maximum(jnp.max(sc, -1, keepdims=True), jnp.max(fs, -1, keepdims=True))
            se = jnp.exp(sc - top)
            fe = jnp.exp(fs - top)
            inv = 1.0 / (jnp.sum(se, -1, keepdims=True) + jnp.sum(fe, -1, keepdims=True))
            prb[i * 2 + s] = (se * inv).astype(BF)
            fresh[i, s] = (fe * inv).astype(BF)
        for i, s in rows:
            if s == 0:
                kvcp[i][1].wait()
            r = slice(s * 8, s * 8 + 8)
            nvb = nv[blocks[i]].astype(F32)
            mix = lax.dot_general(
                prb[i * 2 + s], vc[i, s], (((1,), (1,)), ((), ())), preferred_element_type=F32
            ) + jnp.dot(fresh[i, s], nvb[r].astype(BF), preferred_element_type=F32)
            mixes.append(jnp.concatenate([mix[h * 8 : h * 8 + 8] for h in range(8)], 1))
        return jnp.concatenate(mixes, 0).astype(BF)

    COLS = [(0, 1024), (1024, 2048), (2048, DP)]
    wo[pl.ds(D, DP - D)] = jnp.zeros((DP - D, 512), BF)

    def project(att, k):
        c0, c1 = COLS[k]
        return lax.dot_general(
            att, wo[pl.ds(c0, c1 - c0)], (((1,), (1,)), ((), ())), preferred_element_type=F32
        ).astype(BF)

    c0 = [[] for _ in range(K)]

    def send_part(d, k):
        cols = pl.ds(COLS[k][0], COLS[k][1] - COLS[k][0])
        c0[k].append(
            rcopy(part.at[d, :, cols], r0.at[d - 1, :, cols], s0s.at[d - 1, k], s0r.at[d - 1, k], ydev(d))
        )

    with jax.named_scope("in0"):
        for cp in incp[:3]:
            cp.wait()
    with jax.named_scope("at0"):
        att = attend((0, 1, 2))
        for cp in wcp:
            cp.start()
    for k in range(K):
        with jax.named_scope(f"wo{k}"):
            if k == 0:
                wocp.wait()
            three = project(att, k)
            for i in range(3):
                part[turns[i], :, COLS[k][0] : COLS[k][1]] = three[i * ROWS : (i + 1) * ROWS]
        if k == 0:
            with jax.named_scope("bar"):
                pl.semaphore_wait(barrier, len(LINES) + len(CROSS))
                for dev in CROSS:
                    pl.semaphore_signal(met, inc=1, device_id=dev, device_id_type=MESH)
        for d in turns[:3]:
            send_part(d, k)
        started += c0[k]
    with jax.named_scope("at2"):
        att = attend((3,))
        for cp in incp[3:]:
            cp.wait()
    with jax.named_scope("wo9"):
        for k in range(K):
            part[0, :, COLS[k][0] : COLS[k][1]] = project(att, k)

    own_r = lax.broadcasted_iota(jnp.int32, (ROWS, NY * ROWS), 0) + y * ROWS
    own_c = lax.broadcasted_iota(jnp.int32, (ROWS, NY * ROWS), 1)
    own = jnp.where(own_r == own_c, 1.0, 0.0).astype(BF)
    rt = lax.dot_general(
        own, routes[...].astype(F32).astype(BF), (((1,), (1,)), ((), ())),
        preferred_element_type=F32,
    )
    lane = lax.broadcasted_iota(jnp.int32, (ROWS, SLOTS), 1)
    lane_f = (lane // 2).astype(F32)
    member = jnp.zeros((ROWS, SLOTS), F32)
    for r in range(4):
        member = member + jnp.where(rt[:, r : r + 1] == lane_f, 1.0, 0.0)
    ti = lax.broadcasted_iota(jnp.int32, (ROWS, ROWS), 0)
    tj = lax.broadcasted_iota(jnp.int32, (ROWS, ROWS), 1)
    lower = jnp.where(tj < ti, 1.0, 0.0).astype(BF)
    rank = jnp.dot(lower, member.astype(BF), preferred_element_type=F32)
    here = (member > 0.5) & (jnp.abs(rank - (lane % 2).astype(F32)) < 0.5)
    one_hot = jnp.where(here, 1.0, 0.0)

    er = lax.broadcasted_iota(jnp.int32, (SLOTS, 1024), 0)
    ec = lax.broadcasted_iota(jnp.int32, (SLOTS, 1024), 1)
    expand = jnp.where(er == (ec // 16) * 2 + ec % 2, 1.0, 0.0).astype(BF)
    same_g = er // ROWS == (ec // 2) % 8

    def spread_out(v):
        wide = jnp.dot(v, expand, preferred_element_type=F32)
        return jnp.where(same_g, jnp.concatenate([wide] * 8, 0), 0.0)

    pick = spread_out(one_hot.astype(BF)).T.astype(BF)

    pr = lax.broadcasted_iota(jnp.int32, (SLOTS, SLOTS), 0)
    pc = lax.broadcasted_iota(jnp.int32, (SLOTS, SLOTS), 1)
    swap = jnp.where(pc == ((pr // 2) % 8) * 16 + (pr // 16) * 2 + pr % 2, 1.0, 0.0).astype(BF)
    wd[pl.ds(D, DP - D)] = jnp.zeros((DP - D, FF), BF)

    first = [int(st[1]) for st in ORDER[: [st[0] for st in ORDER].index("y")] if st[0] == "s"]
    pl.semaphore_wait(met, len(CROSS))
    square = 0.0
    for k in range(K):
        lo_, hi_ = COLS[k][0], min(COLS[k][1], D)
        with jax.named_scope(f"w{k}"):
            for cp in c0[k]:
                cp.wait_recv()
        resid = hid[y, :, lo_:hi_].astype(F32) + (
            part[0, :, lo_:hi_].astype(F32) + r0[0, :, lo_:hi_].astype(F32)
            + r0[1, :, lo_:hi_].astype(F32) + r0[2, :, lo_:hi_].astype(F32)
        )
        res[:, lo_:hi_] = resid
        square = square + jnp.sum(resid * resid, -1, keepdims=True)
        if k == K - 1:
            unit = lax.rsqrt(square / D + 1e-05)
            unit_hi = unit.astype(BF).astype(F32)
            spare = lax.broadcasted_iota(jnp.int32, (ROWS, 1024), 1)
            resid = jnp.concatenate([resid, jnp.zeros((ROWS, PAD - D), F32)], 1)
            resid = jnp.where(
                spare == D - lo_, unit_hi, jnp.where(spare == D - lo_ + 1, unit - unit_hi, resid)
            )
        nrm[:, k * 1024 : k * 1024 + 1024] = resid.astype(BF)
        tok = jnp.concatenate(
            [nrm[:, k * 1024 + g * 128 : k * 1024 + g * 128 + 128] for g in range(8)], 0
        )
        rows = jnp.dot(pick, tok, preferred_element_type=F32)
        zs[:, k] = rows.astype(BF).reshape(64, ROWS, 128)
        for n in first:
            for p, i in PEERS:
                if CLASSES[n][0] <= p < CLASSES[n][1]:
                    e = eidx(JZ[p], i)
                    rcopy(zs.at[e, k], xr.at[p, i, k], zss.at[0], zsr.at[p], (e, y))
    xr[0, 0] = zs[ep]

    def stage_s(n):
        for p, i in PEERS:
            if n not in first and CLASSES[n][0] <= p < CLASSES[n][1]:
                e = eidx(JZ[p], i)
                rcopy(zs.at[e], xr.at[p, i], zss.at[0], zsr.at[p], (e, y))

    def arrived(sem, n):
        pltpu.make_async_remote_copy(
            src_ref=zs.at[pl.ds(0, n)], dst_ref=rr.at[pl.ds(0, n)], send_sem=zss.at[0],
            recv_sem=sem, device_id=(ep, (y + 1) % NY), device_id_type=MESH,
        ).wait_recv()

    def sent(sem, n):
        pltpu.make_async_remote_copy(
            src_ref=zs.at[pl.ds(0, n)], dst_ref=rr.at[pl.ds(0, n)], send_sem=sem,
            recv_sem=zsr.at[0], device_id=(ep, (y + 1) % NY), device_id_type=MESH,
        ).wait_send()

    def group(p):
        return NXC - 1 if p == 0 else NXC

    late = {}

    def weigh(_):
        wcp[0].wait()
        logits = lax.dot_general(
            nrm[:, 0:D], wr[...], (((1,), (1,)), ((), ())), preferred_element_type=F32
        ) * unit
        le = lax.broadcasted_iota(jnp.int32, (64, SLOTS), 0)
        ls = lax.broadcasted_iota(jnp.int32, (64, SLOTS), 1)
        spread = jnp.where(le == ls // 2, 1.0, 0.0)
        logits = jnp.dot(
            logits, spread, preferred_element_type=F32, precision=lax.Precision.HIGHEST
        )
        picked = jnp.where(here, jnp.exp(logits), 0.0)
        weight = picked / jnp.sum(picked, -1, keepdims=True)
        hi = weight.astype(BF)
        late["hi"] = spread_out(hi).astype(BF)
        late["lo"] = spread_out((weight - hi.astype(F32)).astype(BF)).astype(BF)

    cy, cf, ca, cb = {}, {}, {}, {}

    def tiles():
        return [(k, g) for k in range(K) for g in range(8) if k * 8 + g < DP // 128]

    def stage_y(i):
        p0, p1 = CLASSES[i]
        ps = pl.ds(p0, p1 - p0)
        for p in range(p0, p1):
            arrived(zsr.at[p], group(p))
            blk = jnp.concatenate([xr[p, :, k].reshape(SLOTS, 128) for k in range(K)], 1)
            r = jnp.dot(swap, blk, preferred_element_type=F32).astype(BF)
            for k, g in tiles():
                t = (k * 8 + g) * 128
                xn[0, p, :, t : t + 128] = r[g * ROWS : (g + 1) * ROWS, k * 128 : k * 128 + 128]
        cy[i] = [
            rcopy(xn.at[0, ps], xn.at[1, ps], yss.at[i, 0], ysr.at[i, 0], ydev(1)),
            rcopy(xn.at[0, ps], xn.at[3, ps], yss.at[i, 1], ysr.at[i, 1], ydev(3)),
        ]
        started.extend(cy[i])

    lo, hi = pl.ds(0, CUT), pl.ds(CUT, DP - CUT)

    def stage_f(i):
        p0, p1 = CLASSES[i]
        ps = pl.ds(p0, p1 - p0)
        cy[i][0].wait_recv()
        a = rcopy(xn.at[1, ps, :, lo], xn.at[2, ps, :, lo], yss.at[i, 2], ysr.at[i, 2], ydev(1))
        cy[i][1].wait_recv()
        b = rcopy(xn.at[3, ps, :, hi], xn.at[2, ps, :, hi], yss.at[i, 3], ysr.at[i, 3], ydev(3))
        cf[i] = [a, b]
        started.extend(cf[i])

    def stage_m(i):
        i0, i1 = MULS[i]
        p0, p1 = CLASSES[i0][0], CLASSES[i1 - 1][1]
        n = p1 - p0
        for j in range(i0, i1):
            for cp in cf[j]:
                cp.wait_recv()
        while len(wcp) > 1:
            wcp.pop().wait()

        rows = xn[:, p0:p1, :, 0:D].reshape(NY * n * ROWS, D)
        u = xn[:, p0:p1, :, D:DP].reshape(NY * n * ROWS, DP - D).astype(F32)
        h = jnp.dot(rows, wgu[...], preferred_element_type=F32) * (u[:, 0:1] + u[:, 1:2])
        gate, up = h[:, 0:FF], h[:, FF : 2 * FF]
        act = ((up + 1.0) * gate * jax.nn.sigmoid(1.702 * gate)).astype(BF)
        o = lax.dot_general(act, wd[...], (((1,), (1,)), ((), ())), preferred_element_type=F32)
        po[:, p0:p1] = o.astype(BF).reshape(NY, n, ROWS, DP)

    def ret_a(i):
        p0, p1 = CLASSES[i]
        ps = pl.ds(p0, p1 - p0)
        ca[i] = [
            rcopy(po.at[2, ps, :, lo], ra1.at[ps], ras.at[i, 0], rar.at[i, 0], ydev(1)),
            rcopy(po.at[2, ps, :, hi], ra2.at[ps], ras.at[i, 1], rar.at[i, 1], ydev(3)),
        ]
        started.extend(ca[i])

    def ret_b(i):
        p0, p1 = CLASSES[i]
        ps = pl.ds(p0, p1 - p0)
        ca[i][0].wait_recv()
        po[3, ps, :, lo] = (po[3, ps, :, lo].astype(F32) + ra1[ps].astype(F32)).astype(BF)
        a = rcopy(po.at[3, ps], rb.at[0, ps], rbs.at[i, 0], rbr.at[i, 0], ydev(1))
        ca[i][1].wait_recv()
        po[1, ps, :, hi] = (po[1, ps, :, hi].astype(F32) + ra2[ps].astype(F32)).astype(BF)
        b = rcopy(po.at[1, ps], rb.at[1, ps], rbs.at[i, 1], rbr.at[i, 1], ydev(3))
        cb[i] = [a, b]
        started.extend(cb[i])

    def ret_x(i):
        p0, p1 = CLASSES[i]
        for cp in cb[i]:
            cp.wait_recv()
        for p in range(p0, p1):
            tot = (
                po[0, p].astype(F32) + rb[0, p].astype(F32) + rb[1, p].astype(F32)
            ).astype(BF)
            tot = jnp.concatenate([tot, jnp.zeros((ROWS, PAD - DP), BF)], 1)
            blk = jnp.concatenate(
                [
                    jnp.concatenate(
                        [tot[:, k * 1024 + g * 128 : k * 1024 + g * 128 + 128] for g in range(8)], 0
                    )
                    for k in range(K)
                ],
                1,
            )
            r = jnp.dot(swap, blk, preferred_element_type=F32).astype(BF)
            for k in range(K):
                ys[p, :, k] = r[:, k * 128 : k * 128 + 128].reshape(NXC, ROWS, 128)
            for j in FAR:
                if (p, j) != (0, 0):
                    rcopy(
                        ys.at[p, j], rr.at[ep], xss.at[0], xsr.at[p],
                        (eidx(JZ[p], j, -1), y),
                    )
        if p0 == 0:
            rr[ep] = ys[0, 0]

    steps = {"s": stage_s, "y": stage_y, "f": stage_f, "m": stage_m, "w": weigh, "a": ret_a, "b": ret_b, "x": ret_x}
    for step in ORDER:
        with jax.named_scope(f"d{step}"):
            steps[step[0]](int(step[1]))

    with jax.named_scope("wr"):
        for p in range(NZ):
            arrived(xsr.at[p], group(p))
    for k in range(K):
        rows = rr[:, k].reshape(1024, 128)
        mix = jnp.dot(late["hi"], rows, preferred_element_type=F32) + jnp.dot(
            late["lo"], rows, preferred_element_type=F32
        )
        for g in range(8):
            c0_ = k * 1024 + g * 128
            c1_ = min(c0_ + 128, D)
            if c1_ > c0_:
                out[:, c0_:c1_] = (
                    res[:, c0_:c1_] + mix[g * ROWS : (g + 1) * ROWS, 0 : c1_ - c0_]
                )

    sent(zss.at[0], NZ * NXC - 1)
    sent(xss.at[0], NZ * NXC - 1)
    for cp in started:
        cp.wait_send()


def moe(*args):
    vm = pl.BlockSpec(memory_space=pltpu.VMEM)
    hbm = pl.BlockSpec(memory_space=pl.ANY)

    n = len(CLASSES)
    dma = pltpu.SemaphoreType.DMA
    return pl.pallas_call(
        moe_kernel,
        out_shape=jax.ShapeDtypeStruct((ROWS, D), F32),
        in_specs=[pl.BlockSpec(memory_space=pltpu.SMEM)] + [hbm] * 12,
        out_specs=vm,
        scratch_shapes=[
            pltpu.VMEM((NY, ROWS, 512), BF),
            pltpu.VMEM((NY, ROWS, 64), BF),
            pltpu.VMEM((NY, ROWS, 64), BF),
            pltpu.VMEM((NY, ROWS, D), BF),
            pltpu.VMEM((4, NY * ROWS), jnp.int32),
            pltpu.VMEM((8, 64, LEN), F32),
            pltpu.VMEM((8, 64, LEN), BF),
            pltpu.VMEM((NY, 2, 64, LEN), BF),
            pltpu.VMEM((NY, 2, 64, LEN), BF),
            pltpu.VMEM((DP, 512), BF),
            pltpu.VMEM((NY, ROWS, DP), BF),
            pltpu.VMEM((64, D), BF),
            pltpu.VMEM((D, 2 * FF), BF),
            pltpu.VMEM((DP, FF), BF),
            pltpu.VMEM((3, ROWS, DP), BF),
            pltpu.VMEM((ROWS, D), F32),
            pltpu.VMEM((ROWS, PAD), BF),
            pltpu.VMEM((NZ * NXC, K, ROWS, 128), BF),
            pltpu.VMEM((NZ, NXC, K, ROWS, 128), BF),
            pltpu.VMEM((NY, NZ, ROWS, DP), BF),
            pltpu.VMEM((NY, NZ, ROWS, DP), BF),
            pltpu.VMEM((NZ, ROWS, CUT), BF),
            pltpu.VMEM((NZ, ROWS, DP - CUT), BF),
            pltpu.VMEM((2, NZ, ROWS, DP), BF),
            pltpu.VMEM((NZ, NXC, K, ROWS, 128), BF),
            pltpu.VMEM((NZ * NXC, K, ROWS, 128), BF),
            pltpu.SemaphoreType.REGULAR,
            dma((5,)),
            dma((2, NY)),
            dma((5,)),
            dma((3, K)), dma((3, K)),
            dma((1,)), dma((NZ,)),
            dma((n, 4)), dma((n, 4)),
            dma((n, 2)), dma((n, 2)),
            dma((n, 2)), dma((n, 2)),
            dma((1,)), dma((NZ,)),
        ],
        compiler_params=pltpu.CompilerParams(
            collective_id=0, has_side_effects=True, vmem_limit_bytes=56 * 1024 * 1024
        ),
    )(*args)


def body(
    hidden,
    queries,
    new_keys,
    new_values,
    key_cache,
    value_cache,
    cache_lengths,
    w_out,
    w_router,
    routes,
    w_gate,
    w_up,
    w_down,
):
    return moe(
        cache_lengths,
        queries.reshape(NY, ROWS, 512),
        new_keys.reshape(NY, ROWS, 64),
        new_values.reshape(NY, ROWS, 64),
        hidden.reshape(NY, ROWS, D),
        routes.T,
        key_cache,
        value_cache,
        w_out.T,
        w_router.T,
        w_gate,
        w_up,
        w_down.transpose(0, 2, 1),
    ).astype(BF)


def solution(mesh):
    return jax.shard_map(
        body,
        mesh=mesh,
        in_specs=(
            P("ep", None),
            P("ep", "tp"),
            P("ep", "tp"),
            P("ep", "tp"),
            P("ep", "tp", None, None),
            P("ep", "tp", None, None),
            P("ep"),
            P("tp", None),
            P(),
            P("ep", None),
            P("ep", None, "tp"),
            P("ep", None, "tp"),
            P("ep", "tp", None),
        ),
        out_specs=P(("ep", "tp"), None),
        check_vma=False,
    )
```

```python
import jax
import jax.numpy as jnp
from jax import lax
from jax.experimental import pallas as pl
from jax.experimental.pallas import tpu as pltpu
from jax.sharding import PartitionSpec as P

MESH = pl.DeviceIdType.MESH
NZ, NX, NC, NY = 8, 4, 2, 4
NXC = NX * NC
D = 2880
FF = 384
LEN = 1024
ROWS = 16
SLOTS = 128
K = 3
PAD = K * 1024
DP = 2944
CUT = 1536
GROUPS = ((0,), (1,), (7,), (3,), (5,), (4,), (2,), (6,))
MULS = ((0, 1, 2), (3, 4), (5, 6, 7))
ORDER = (
    "s4", "s3", "s0", "y0", "s6", "s1", "y4", "s7", "f0", "s5", "y3", "f4",
    "s2", "y6", "w0", "y1", "f3", "y7", "f6", "y5", "y2", "m1", "a3", "f7",
    "f5", "a4", "f1", "f2", "b3", "m2", "a6", "a5", "b4", "m0", "a2", "a7",
    "x3", "b5", "b6", "x4", "a1", "b2", "a0", "x5", "b7", "b1", "x6", "b0",
    "x2", "x7", "x1", "x0",
)
JZ = tuple(j for g in GROUPS for j in g)
CLASSES = tuple((sum(map(len, GROUPS[:i])), sum(map(len, GROUPS[: i + 1]))) for i in range(len(GROUPS)))
MULS = tuple((m[0], m[-1] + 1) for m in MULS)
BF = jnp.bfloat16
F32 = jnp.float32


def moe_kernel(
    lens, q_h, nk_h, nv_h, hid_h, rt_h, kc_h, vc_h, wo_h, wr_h, wg_h, wu_h, wd_h, out,
    q, nk, nv, hid, routes, sco, prb, kc, vc, wo, part, wr, wgu, wd, r0, res, nrm, zs, xr, xn, po, ra1, ra2, rb, ys, rr, wsp,
    met, in_sem, kv_sem, w_sem, s0s, s0r, zss, zsr, yss, ysr, ras, rar, rbs, rbr, xss, xsr,
):
    ep = lax.axis_index("ep")
    y = lax.axis_index("tp")
    c = ep % NC
    x = (ep // NC) % NX
    z = ep // NXC
    xc = x * NC + c

    turns = (2, 1, 3, 0)
    blocks = [(y + d) % NY for d in turns]
    kvcp = []
    for i, b in enumerate(blocks):
        two = pl.ds(b * 2, 2)
        kvcp.append((
            pltpu.make_async_copy(kc_h.at[two, 0], kc.at[i], kv_sem.at[0, i]),
            pltpu.make_async_copy(vc_h.at[two, 0], vc.at[i], kv_sem.at[1, i]),
        ))
    wocp = pltpu.make_async_copy(wo_h, wo.at[pl.ds(0, D)], w_sem.at[4])
    wcp = [
        pltpu.make_async_copy(wr_h, wr, w_sem.at[0]),
        pltpu.make_async_copy(wg_h.at[0], wgu.at[:, pl.ds(0, FF)], w_sem.at[1]),
        pltpu.make_async_copy(wu_h.at[0], wgu.at[:, pl.ds(FF, FF)], w_sem.at[2]),
        pltpu.make_async_copy(wd_h.at[0], wd.at[pl.ds(0, D)], w_sem.at[3]),
    ]
    small = [(q_h, q), (nk_h, nk), (nv_h, nv), (rt_h, routes), (hid_h, hid)]
    incp = [pltpu.make_async_copy(a, b, in_sem.at[i]) for i, (a, b) in enumerate(small)]
    incp[0].start()
    for pair in kvcp[:3]:
        pair[0].start()
    for cp in incp[1:3]:
        cp.start()
    for pair in kvcp[:3]:
        pair[1].start()
    wocp.start()
    for cp in kvcp[3]:
        cp.start()
    for cp in incp[3:]:
        cp.start()

    def eidx(jz, i, sign=1):
        jx, jc = sign * (i // NC), i % NC
        return ((z + sign * jz) % NZ) * NXC + ((x + jx) % NX) * NC + (c + jc) % NC

    def ydev(d):
        return (ep, (y + d) % NY)

    FAR = (4, 5, 2, 3, 6, 7, 1, 0)
    PEERS = [(p, i) for p in range(NZ) for i in FAR if (p, i) != (0, 0)]

    barrier = pltpu.get_barrier_semaphore()
    LINES = [(eidx(j, 0), y) for j in range(1, NZ)] + [ydev(d) for d in range(1, NY)]
    CROSS = [(eidx(0, i), y) for i in FAR if i]
    for dev in LINES + CROSS:
        pl.semaphore_signal(barrier, inc=1, device_id=dev, device_id_type=MESH)

    def rcopy(src, dst, ssem, rsem, dev):
        cp = pltpu.make_async_remote_copy(
            src_ref=src, dst_ref=dst, send_sem=ssem, recv_sem=rsem,
            device_id=dev, device_id_type=MESH,
        )
        cp.start()
        return cp

    started = []

    pos = lax.broadcasted_iota(jnp.int32, (64, LEN), 1)
    causal = (
        lax.broadcasted_iota(jnp.int32, (64, 8), 0) % 8
        >= lax.broadcasted_iota(jnp.int32, (64, 8), 1)
    )
    scale = 64 ** (-0.5)

    def attend(which):
        rows = [(i, s) for i in which for s in range(2)]
        fresh, mixes = {}, []
        for i, s in rows:
            if s == 0:
                kvcp[i][0].wait()
            b = blocks[i]
            r = slice(s * 8, s * 8 + 8)
            qb, nkb = q[b].astype(F32), nk[b].astype(F32)
            qs = jnp.concatenate([qb[r, h * 64 : h * 64 + 64] for h in range(8)], 0).astype(BF)
            sc = jnp.dot(qs, kc[i, s], preferred_element_type=F32) * scale
            sco[i * 2 + s] = jnp.where(pos < lens[b * 2 + s], sc, -1e30)
            fs = lax.dot_general(
                qs, nkb[r].astype(BF), (((1,), (1,)), ((), ())), preferred_element_type=F32
            ) * scale
            fresh[i, s] = jnp.where(causal, fs, -1e30)
        for i, s in rows:
            sc, fs = sco[i * 2 + s], fresh[i, s]
            top = jnp.maximum(jnp.max(sc, -1, keepdims=True), jnp.max(fs, -1, keepdims=True))
            se = jnp.exp(sc - top)
            fe = jnp.exp(fs - top)
            inv = 1.0 / (jnp.sum(se, -1, keepdims=True) + jnp.sum(fe, -1, keepdims=True))
            prb[i * 2 + s] = (se * inv).astype(BF)
            fresh[i, s] = (fe * inv).astype(BF)
        for i, s in rows:
            if s == 0:
                kvcp[i][1].wait()
            r = slice(s * 8, s * 8 + 8)
            nvb = nv[blocks[i]].astype(F32)
            mix = lax.dot_general(
                prb[i * 2 + s], vc[i, s], (((1,), (1,)), ((), ())), preferred_element_type=F32
            ) + jnp.dot(fresh[i, s], nvb[r].astype(BF), preferred_element_type=F32)
            mixes.append(jnp.concatenate([mix[h * 8 : h * 8 + 8] for h in range(8)], 1))
        return jnp.concatenate(mixes, 0).astype(BF)

    COLS = [(0, 1024), (1024, 2048), (2048, DP)]
    wo[pl.ds(D, DP - D)] = jnp.zeros((DP - D, 512), BF)

    def project(att, k):
        c0, c1 = COLS[k]
        return lax.dot_general(
            att, wo[pl.ds(c0, c1 - c0)], (((1,), (1,)), ((), ())), preferred_element_type=F32
        ).astype(BF)

    c0 = [[] for _ in range(K)]

    def send_part(d, k):
        cols = pl.ds(COLS[k][0], COLS[k][1] - COLS[k][0])
        c0[k].append(
            rcopy(part.at[d, :, cols], r0.at[d - 1, :, cols], s0s.at[d - 1, k], s0r.at[d - 1, k], ydev(d))
        )

    with jax.named_scope("in0"):
        for cp in incp[:3]:
            cp.wait()
    with jax.named_scope("at0"):
        att = attend((0, 1, 2))
        for cp in wcp:
            cp.start()
    for k in range(K):
        with jax.named_scope(f"wo{k}"):
            if k == 0:
                wocp.wait()
            three = project(att, k)
            for i in range(3):
                part[turns[i], :, COLS[k][0] : COLS[k][1]] = three[i * ROWS : (i + 1) * ROWS]
        if k == 0:
            with jax.named_scope("bar"):
                pl.semaphore_wait(barrier, len(LINES) + len(CROSS))
                for dev in CROSS:
                    pl.semaphore_signal(met, inc=1, device_id=dev, device_id_type=MESH)
        for d in turns[:3]:
            send_part(d, k)
        started += c0[k]
    with jax.named_scope("at2"):
        att = attend((3,))
        for cp in incp[3:]:
            cp.wait()
    with jax.named_scope("wo9"):
        for k in range(K):
            part[0, :, COLS[k][0] : COLS[k][1]] = project(att, k)

    own_r = lax.broadcasted_iota(jnp.int32, (ROWS, NY * ROWS), 0) + y * ROWS
    own_c = lax.broadcasted_iota(jnp.int32, (ROWS, NY * ROWS), 1)
    own = jnp.where(own_r == own_c, 1.0, 0.0).astype(BF)
    rt = lax.dot_general(
        own, routes[...].astype(F32).astype(BF), (((1,), (1,)), ((), ())),
        preferred_element_type=F32,
    )
    lane = lax.broadcasted_iota(jnp.int32, (ROWS, SLOTS), 1)
    lane_f = (lane // 2).astype(F32)
    member = jnp.zeros((ROWS, SLOTS), F32)
    for r in range(4):
        member = member + jnp.where(rt[:, r : r + 1] == lane_f, 1.0, 0.0)
    ti = lax.broadcasted_iota(jnp.int32, (ROWS, ROWS), 0)
    tj = lax.broadcasted_iota(jnp.int32, (ROWS, ROWS), 1)
    lower = jnp.where(tj < ti, 1.0, 0.0).astype(BF)
    rank = jnp.dot(lower, member.astype(BF), preferred_element_type=F32)
    here = (member > 0.5) & (jnp.abs(rank - (lane % 2).astype(F32)) < 0.5)
    one_hot = jnp.where(here, 1.0, 0.0)

    er = lax.broadcasted_iota(jnp.int32, (SLOTS, 1024), 0)
    ec = lax.broadcasted_iota(jnp.int32, (SLOTS, 1024), 1)
    expand = jnp.where(er == (ec // 16) * 2 + ec % 2, 1.0, 0.0).astype(BF)
    same_g = er // ROWS == (ec // 2) % 8

    def spread_out(v):
        wide = jnp.dot(v, expand, preferred_element_type=F32)
        return jnp.where(same_g, jnp.concatenate([wide] * 8, 0), 0.0)

    pick = spread_out(one_hot.astype(BF)).T.astype(BF)

    pr = lax.broadcasted_iota(jnp.int32, (SLOTS, SLOTS), 0)
    pc = lax.broadcasted_iota(jnp.int32, (SLOTS, SLOTS), 1)
    swap = jnp.where(pc == ((pr // 2) % 8) * 16 + (pr // 16) * 2 + pr % 2, 1.0, 0.0).astype(BF)
    wd[pl.ds(D, DP - D)] = jnp.zeros((DP - D, FF), BF)

    first = [int(st[1]) for st in ORDER[: [st[0] for st in ORDER].index("y")] if st[0] == "s"]
    pl.semaphore_wait(met, len(CROSS))
    square = 0.0
    for k in range(K):
        lo_, hi_ = COLS[k][0], min(COLS[k][1], D)
        with jax.named_scope(f"w{k}"):
            for cp in c0[k]:
                cp.wait_recv()
        resid = hid[y, :, lo_:hi_].astype(F32) + (
            part[0, :, lo_:hi_].astype(F32) + r0[0, :, lo_:hi_].astype(F32)
            + r0[1, :, lo_:hi_].astype(F32) + r0[2, :, lo_:hi_].astype(F32)
        )
        res[:, lo_:hi_] = resid
        square = square + jnp.sum(resid * resid, -1, keepdims=True)
        if k == K - 1:
            unit = lax.rsqrt(square / D + 1e-05)
            unit_hi = unit.astype(BF).astype(F32)
            spare = lax.broadcasted_iota(jnp.int32, (ROWS, 1024), 1)
            resid = jnp.concatenate([resid, jnp.zeros((ROWS, PAD - D), F32)], 1)
            resid = jnp.where(
                spare == D - lo_, unit_hi, jnp.where(spare == D - lo_ + 1, unit - unit_hi, resid)
            )
        nrm[:, k * 1024 : k * 1024 + 1024] = resid.astype(BF)
        tok = jnp.concatenate(
            [nrm[:, k * 1024 + g * 128 : k * 1024 + g * 128 + 128] for g in range(8)], 0
        )
        rows = jnp.dot(pick, tok, preferred_element_type=F32)
        zs[:, k] = rows.astype(BF).reshape(64, ROWS, 128)
        for n in first:
            for p, i in PEERS:
                if CLASSES[n][0] <= p < CLASSES[n][1]:
                    e = eidx(JZ[p], i)
                    rcopy(zs.at[e, k], xr.at[p, i, k], zss.at[0], zsr.at[p], (e, y))
    xr[0, 0] = zs[ep]

    def stage_s(n):
        for p, i in PEERS:
            if n not in first and CLASSES[n][0] <= p < CLASSES[n][1]:
                e = eidx(JZ[p], i)
                rcopy(zs.at[e], xr.at[p, i], zss.at[0], zsr.at[p], (e, y))

    def arrived(sem, n):
        pltpu.make_async_remote_copy(
            src_ref=zs.at[pl.ds(0, n)], dst_ref=rr.at[pl.ds(0, n)], send_sem=zss.at[0],
            recv_sem=sem, device_id=(ep, (y + 1) % NY), device_id_type=MESH,
        ).wait_recv()

    def sent(sem, n):
        pltpu.make_async_remote_copy(
            src_ref=zs.at[pl.ds(0, n)], dst_ref=rr.at[pl.ds(0, n)], send_sem=sem,
            recv_sem=zsr.at[0], device_id=(ep, (y + 1) % NY), device_id_type=MESH,
        ).wait_send()

    def group(p):
        return NXC - 1 if p == 0 else NXC


    def weigh(_):
        wcp[0].wait()
        logits = lax.dot_general(
            nrm[:, 0:D], wr[...], (((1,), (1,)), ((), ())), preferred_element_type=F32
        ) * unit
        le = lax.broadcasted_iota(jnp.int32, (64, SLOTS), 0)
        ls = lax.broadcasted_iota(jnp.int32, (64, SLOTS), 1)
        spread = jnp.where(le == ls // 2, 1.0, 0.0)
        logits = jnp.dot(
            logits, spread, preferred_element_type=F32, precision=lax.Precision.HIGHEST
        )
        picked = jnp.where(here, jnp.exp(logits), 0.0)
        weight = picked / jnp.sum(picked, -1, keepdims=True)
        hi = weight.astype(BF)
        wsp[0:SLOTS] = spread_out(hi).astype(BF)
        wsp[SLOTS:] = spread_out((weight - hi.astype(F32)).astype(BF)).astype(BF)

    cy, cf, ca, cb = {}, {}, {}, {}

    def tiles():
        return [(k, g) for k in range(K) for g in range(8) if k * 8 + g < DP // 128]

    def stage_y(i):
        p0, p1 = CLASSES[i]
        ps = pl.ds(p0, p1 - p0)
        for p in range(p0, p1):
            arrived(zsr.at[p], group(p))
            blk = jnp.concatenate([xr[p, :, k].reshape(SLOTS, 128) for k in range(K)], 1)
            r = jnp.dot(swap, blk, preferred_element_type=F32).astype(BF)
            for k, g in tiles():
                t = (k * 8 + g) * 128
                xn[0, p, :, t : t + 128] = r[g * ROWS : (g + 1) * ROWS, k * 128 : k * 128 + 128]
        cy[i] = [
            rcopy(xn.at[0, ps], xn.at[1, ps], yss.at[i, 0], ysr.at[i, 0], ydev(1)),
            rcopy(xn.at[0, ps], xn.at[3, ps], yss.at[i, 1], ysr.at[i, 1], ydev(3)),
        ]
        started.extend(cy[i])

    def halves(i):
        both = (pl.ds(0, CUT), pl.ds(CUT, DP - CUT))
        return both if i % 2 == 0 else both[::-1]

    def stage_f(i):
        p0, p1 = CLASSES[i]
        ps = pl.ds(p0, p1 - p0)
        lo, hi = halves(i)
        cy[i][0].wait_recv()
        a = rcopy(xn.at[1, ps, :, lo], xn.at[2, ps, :, lo], yss.at[i, 2], ysr.at[i, 2], ydev(1))
        cy[i][1].wait_recv()
        b = rcopy(xn.at[3, ps, :, hi], xn.at[2, ps, :, hi], yss.at[i, 3], ysr.at[i, 3], ydev(3))
        cf[i] = [a, b]
        started.extend(cf[i])

    def stage_m(i):
        i0, i1 = MULS[i]
        p0, p1 = CLASSES[i0][0], CLASSES[i1 - 1][1]
        n = p1 - p0
        for j in range(i0, i1):
            for cp in cf[j]:
                cp.wait_recv()
        while len(wcp) > 1:
            wcp.pop().wait()

        rows = xn[:, p0:p1, :, 0:D].reshape(NY * n * ROWS, D)
        u = xn[:, p0:p1, :, D:DP].reshape(NY * n * ROWS, DP - D).astype(F32)
        h = jnp.dot(rows, wgu[...], preferred_element_type=F32) * (u[:, 0:1] + u[:, 1:2])
        gate, up = h[:, 0:FF], h[:, FF : 2 * FF]
        act = ((up + 1.0) * gate * jax.nn.sigmoid(1.702 * gate)).astype(BF)
        o = lax.dot_general(act, wd[...], (((1,), (1,)), ((), ())), preferred_element_type=F32)
        po[:, p0:p1] = o.astype(BF).reshape(NY, n, ROWS, DP)

    def ret_a(i):
        p0, p1 = CLASSES[i]
        ps = pl.ds(p0, p1 - p0)
        lo, hi = halves(i)
        ca[i] = [
            rcopy(po.at[2, ps, :, lo], ra1.at[ps, :, lo], ras.at[i, 0], rar.at[i, 0], ydev(1)),
            rcopy(po.at[2, ps, :, hi], ra2.at[ps, :, hi], ras.at[i, 1], rar.at[i, 1], ydev(3)),
        ]
        started.extend(ca[i])

    def ret_b(i):
        p0, p1 = CLASSES[i]
        ps = pl.ds(p0, p1 - p0)
        lo, hi = halves(i)
        ca[i][0].wait_recv()
        po[3, ps, :, lo] = (po[3, ps, :, lo].astype(F32) + ra1[ps, :, lo].astype(F32)).astype(BF)
        a = rcopy(po.at[3, ps], rb.at[0, ps], rbs.at[i, 0], rbr.at[i, 0], ydev(1))
        ca[i][1].wait_recv()
        po[1, ps, :, hi] = (po[1, ps, :, hi].astype(F32) + ra2[ps, :, hi].astype(F32)).astype(BF)
        b = rcopy(po.at[1, ps], rb.at[1, ps], rbs.at[i, 1], rbr.at[i, 1], ydev(3))
        cb[i] = [a, b]
        started.extend(cb[i])

    def ret_x(i):
        p0, p1 = CLASSES[i]
        for cp in cb[i]:
            cp.wait_recv()
        for p in range(p0, p1):
            tot = (
                po[0, p].astype(F32) + rb[0, p].astype(F32) + rb[1, p].astype(F32)
            ).astype(BF)
            tot = jnp.concatenate([tot, jnp.zeros((ROWS, PAD - DP), BF)], 1)
            blk = jnp.concatenate(
                [
                    jnp.concatenate(
                        [tot[:, k * 1024 + g * 128 : k * 1024 + g * 128 + 128] for g in range(8)], 0
                    )
                    for k in range(K)
                ],
                1,
            )
            r = jnp.dot(swap, blk, preferred_element_type=F32).astype(BF)
            for k in range(K):
                ys[p, :, k] = r[:, k * 128 : k * 128 + 128].reshape(NXC, ROWS, 128)
            for j in FAR:
                if (p, j) != (0, 0):
                    rcopy(
                        ys.at[p, j], rr.at[ep], xss.at[0], xsr.at[p],
                        (eidx(JZ[p], j, -1), y),
                    )
        if p0 == 0:
            rr[ep] = ys[0, 0]

    steps = {"s": stage_s, "y": stage_y, "f": stage_f, "m": stage_m, "w": weigh, "a": ret_a, "b": ret_b, "x": ret_x}
    for step in ORDER:
        with jax.named_scope(f"d{step}"):
            steps[step[0]](int(step[1]))

    sent(zss.at[0], NZ * NXC - 1)
    for cp in started:
        cp.wait_send()

    total = jnp.zeros((2 * SLOTS, K * 128), F32)
    for n in [int(st[1]) for st in ORDER if st[0] == "x"]:
        for p in range(*CLASSES[n]):
            with jax.named_scope(f"wr{p}"):
                arrived(xsr.at[p], group(p))
            zg = (z + JZ[p]) % NZ
            got = rr[pl.ds(pl.multiple_of(zg * NXC, NXC), NXC)]
            blk = jnp.concatenate([got[:, k].reshape(SLOTS, 128) for k in range(K)], 1)
            total = total + jnp.dot(
                wsp[:, pl.ds(pl.multiple_of(zg * SLOTS, SLOTS), SLOTS)], blk,
                preferred_element_type=F32,
            )
    mix = total[0:SLOTS] + total[SLOTS:]
    with jax.named_scope("fin"):
        for k in range(K):
            for g in range(8):
                c0_ = k * 1024 + g * 128
                c1_ = min(c0_ + 128, D)
                if c1_ > c0_:
                    out[:, c0_:c1_] = res[:, c0_:c1_] + mix[
                        g * ROWS : (g + 1) * ROWS, k * 128 : k * 128 + c1_ - c0_
                    ]

    sent(xss.at[0], NZ * NXC - 1)


def moe(*args):
    vm = pl.BlockSpec(memory_space=pltpu.VMEM)
    hbm = pl.BlockSpec(memory_space=pl.ANY)

    n = len(CLASSES)
    dma = pltpu.SemaphoreType.DMA
    return pl.pallas_call(
        moe_kernel,
        out_shape=jax.ShapeDtypeStruct((ROWS, D), F32),
        in_specs=[pl.BlockSpec(memory_space=pltpu.SMEM)] + [hbm] * 12,
        out_specs=vm,
        scratch_shapes=[
            pltpu.VMEM((NY, ROWS, 512), BF),
            pltpu.VMEM((NY, ROWS, 64), BF),
            pltpu.VMEM((NY, ROWS, 64), BF),
            pltpu.VMEM((NY, ROWS, D), BF),
            pltpu.VMEM((4, NY * ROWS), jnp.int32),
            pltpu.VMEM((8, 64, LEN), F32),
            pltpu.VMEM((8, 64, LEN), BF),
            pltpu.VMEM((NY, 2, 64, LEN), BF),
            pltpu.VMEM((NY, 2, 64, LEN), BF),
            pltpu.VMEM((DP, 512), BF),
            pltpu.VMEM((NY, ROWS, DP), BF),
            pltpu.VMEM((64, D), BF),
            pltpu.VMEM((D, 2 * FF), BF),
            pltpu.VMEM((DP, FF), BF),
            pltpu.VMEM((3, ROWS, DP), BF),
            pltpu.VMEM((ROWS, D), F32),
            pltpu.VMEM((ROWS, PAD), BF),
            pltpu.VMEM((NZ * NXC, K, ROWS, 128), BF),
            pltpu.VMEM((NZ, NXC, K, ROWS, 128), BF),
            pltpu.VMEM((NY, NZ, ROWS, DP), BF),
            pltpu.VMEM((NY, NZ, ROWS, DP), BF),
            pltpu.VMEM((NZ, ROWS, DP), BF),
            pltpu.VMEM((NZ, ROWS, DP), BF),
            pltpu.VMEM((2, NZ, ROWS, DP), BF),
            pltpu.VMEM((NZ, NXC, K, ROWS, 128), BF),
            pltpu.VMEM((NZ * NXC, K, ROWS, 128), BF),
            pltpu.VMEM((2 * SLOTS, 1024), BF),
            pltpu.SemaphoreType.REGULAR,
            dma((5,)),
            dma((2, NY)),
            dma((5,)),
            dma((3, K)), dma((3, K)),
            dma((1,)), dma((NZ,)),
            dma((n, 4)), dma((n, 4)),
            dma((n, 2)), dma((n, 2)),
            dma((n, 2)), dma((n, 2)),
            dma((1,)), dma((NZ,)),
        ],
        compiler_params=pltpu.CompilerParams(
            collective_id=0, has_side_effects=True, vmem_limit_bytes=56 * 1024 * 1024
        ),
    )(*args)


def body(
    hidden,
    queries,
    new_keys,
    new_values,
    key_cache,
    value_cache,
    cache_lengths,
    w_out,
    w_router,
    routes,
    w_gate,
    w_up,
    w_down,
):
    return moe(
        cache_lengths,
        queries.reshape(NY, ROWS, 512),
        new_keys.reshape(NY, ROWS, 64),
        new_values.reshape(NY, ROWS, 64),
        hidden.reshape(NY, ROWS, D),
        routes.T,
        key_cache,
        value_cache,
        w_out.T,
        w_router.T,
        w_gate,
        w_up,
        w_down.transpose(0, 2, 1),
    ).astype(BF)


def solution(mesh):
    return jax.shard_map(
        body,
        mesh=mesh,
        in_specs=(
            P("ep", None),
            P("ep", "tp"),
            P("ep", "tp"),
            P("ep", "tp"),
            P("ep", "tp", None, None),
            P("ep", "tp", None, None),
            P("ep"),
            P("tp", None),
            P(),
            P("ep", None),
            P("ep", None, "tp"),
            P("ep", None, "tp"),
            P("ep", "tp", None),
        ),
        out_specs=P(("ep", "tp"), None),
        check_vma=False,
    )
```
